32 devices in a mesh: expert: 8 (over z, x), dp: 4 (over y, core).
Axes of the slice: x: 2, y: 2, z: 4, core: 2. Of those that a mesh axis runs over, the one named last changes fastest.
Arguments:
- grad_output: bfloat16 [4096, 2048], P(('expert', 'dp')), may hold values from -1.5 to 1.5
- logits: float32 [4096, 8], P(('expert', 'dp')), may hold values from -6 to 6
- chosen: int32 [4096, 8], P(('expert', 'dp')), may hold values from 0 to 31, as said below
- slots: int32 [4096, 8], P(('expert', 'dp')), may hold values from 0 to 40, as said below
- other_scores: float32 [4096, 8], P(('expert', 'dp')), may hold values from -48 to 48
- hidden: bfloat16 [8, 4, 8, 40, 768], P('expert', 'dp'), may hold values from -6 to 6
- down_weight: bfloat16 [8, 768, 2048], P('expert', 'dp'), may hold values from -0.21875 to 0.21875
Outputs:
- grad_hidden: bfloat16 [8, 4, 8, 40, 768], P('expert', 'dp')
- grad_down: float32 [8, 768, 2048], P('expert', 'dp')
- grad_logits: float32 [4096, 8], P(('expert', 'dp'))
The draws below stay inside these ranges and needn't reach their ends.
Inputs may be any that keep to these rules, and one draw needn't show every extreme that they name: `chosen`: each row names 8 different experts. 40 marks a choice with no slot: its expert is 8 or above, or it comes after 40 earlier choices of the same expert among the rows of one device in row-major order. The live choices of one expert on one device hold slots 0, 1, 2, ... in that order. Some expert fills all 40 slots on some device.
All inputs are finite; a program needn't handle non-finite values.
Results may differ from the reference program's by a relative error of at most 0.023.
Values may be sent and summed in bfloat16 or wider, within the bound.
A program may use at most 64 MiB of HBM per device.

```python
import jax
import jax.numpy as jnp
from jax import lax

D = 2048
FF = 768
TOPK = 8
TOK_DEV = 128
EXPERTS = 32
WINDOW = 8
CAP = 40
TOKENS = 4096
N_EXPERT = 8
N_DP = 4


def route_table(key):
    inner_key = jax.random.fold_in(key, 11)
    random_bits = jax.random.randint(inner_key, (TOKENS, EXPERTS), 0, 1 << 20)
    ranking = random_bits * EXPERTS + jnp.arange(EXPERTS, dtype=jnp.int32)[None, :]
    unused, picked = lax.top_k(ranking, TOPK)
    picked = picked.astype(jnp.int32)
    blocks = picked.reshape(TOKENS // TOK_DEV, TOK_DEV * TOPK)
    onehot = (blocks[:, :, None] == jnp.arange(WINDOW, dtype=jnp.int32)[None, None, :]).astype(jnp.int32)
    ranks = jnp.cumsum(onehot, axis=1) - 1
    position = jnp.sum(ranks * onehot, axis=2)
    inside = (blocks < WINDOW) & (position < CAP)
    placed = jnp.where(inside, position, CAP).astype(jnp.int32)
    return (picked, placed.reshape(TOKENS, TOPK))


def draw_chosen(key, part):
    picked, placed = route_table(key)
    return picked


def draw_slots(key, part):
    picked, placed = route_table(key)
    return placed


def block_levels(rng, extent, shards, smallest, top_value):
    def one(dim, shards_of):
        steps = jax.random.uniform(jax.random.fold_in(jax.random.fold_in(rng, 6), dim), (shards_of,), jnp.float32, smallest / len(shards), top_value / len(shards))
        return jnp.repeat(jnp.exp(steps), extent[dim] // shards_of).reshape((-1,) + (1,) * (len(extent) - dim - 1))

    gain = one(*shards[0])
    for cut in shards[1:]:
        gain = gain * one(*cut)
    return gain


def bell_draw(key, shape, width, reach, pieces=(), kind=jnp.bfloat16):
    factor_of = block_levels(key, shape, pieces, -0.22, 0.18) if pieces else 1.0
    values = jax.random.normal(key, shape, jnp.float32) * width * factor_of
    return jnp.minimum(jnp.maximum(values, -reach), reach).astype(kind)


def setup_inputs(seed: int = 0) -> dict:
    streams_of = jax.random.split(jax.random.key(seed), 8)
    return {
        "grad_output": bell_draw(streams_of[0], (TOKENS, D), 0.25, 1.5, ((0, 32),)),
        "logits": bell_draw(streams_of[1], (TOKENS, TOPK), 1.0, 6.0, ((0, 32),), jnp.float32),
        "chosen": draw_chosen(jax.random.fold_in(streams_of[7], 71), 0),
        "slots": draw_slots(jax.random.fold_in(streams_of[7], 71), 0),
        "other_scores": bell_draw(streams_of[4], (TOKENS, TOPK), 8.0, 48.0, ((0, 32),), jnp.float32),
        "hidden": bell_draw(streams_of[5], (WINDOW, N_DP, N_EXPERT, CAP, FF), 1.0, 6.0, ((0, 8), (1, 4))),
        "down_weight": bell_draw(streams_of[6], (WINDOW, FF, D), FF ** -0.5, 0.21875, ((0, 8), (1, 4))),
    }


def reference(grad_output, logits, chosen, slots, other_scores, hidden, down_weight):
    raised = jnp.exp(logits)
    gating = raised / jnp.sum(raised, axis=1, keepdims=True)
    gate_sent = gating.astype(jnp.bfloat16)
    row_index = jnp.arange(TOKENS, dtype=jnp.int32)
    block_index = row_index // TOK_DEV
    source_index = block_index // N_DP
    shard_index = block_index % N_DP
    live_slot = slots < CAP
    slot_count = N_DP * N_EXPERT * CAP
    total_slots = WINDOW * slot_count
    flat_place = ((chosen * N_DP + shard_index[:, None]) * N_EXPERT + source_index[:, None]) * CAP + slots
    flat_place = jnp.where(live_slot, flat_place, total_slots).astype(jnp.int32).reshape(-1)
    pair_index = jnp.arange(TOKENS * TOPK, dtype=jnp.int32)
    owners = jnp.zeros((total_slots + 1,), jnp.int32).at[flat_place].set(pair_index)
    filled = jnp.zeros((total_slots + 1,), jnp.float32).at[flat_place].set(1.0)
    owners = owners[:total_slots].reshape(WINDOW, slot_count)
    filled = filled[:total_slots].reshape(WINDOW, slot_count)
    gate_flat = gate_sent.reshape(-1)

    def expert_pass(inputs):
        owner_rows, fill_rows, expert_hidden, expert_weight = inputs
        slot_mask = fill_rows.astype(jnp.bfloat16)
        slot_rows = grad_output[owner_rows // TOPK] * slot_mask[:, None]
        slot_gate = (gate_flat[owner_rows] * slot_mask).astype(jnp.float32)
        local_hidden = expert_hidden.reshape(slot_count, FF)
        upward = lax.dot_general(slot_rows, expert_weight, (((1,), (1,)), ((), ())), preferred_element_type=jnp.float32)
        grad_rows = (slot_gate[:, None] * upward).astype(jnp.bfloat16)
        outputs = jnp.dot(local_hidden, expert_weight, preferred_element_type=jnp.float32)
        slot_scores = jnp.sum(slot_rows.astype(jnp.float32) * outputs, axis=1)
        scaled = (slot_gate[:, None] * slot_rows.astype(jnp.float32)).astype(jnp.bfloat16)

        def add_shard(totals, shard):
            shard_hidden, shard_scaled = shard
            partial_value = lax.dot_general(shard_hidden, shard_scaled, (((0,), (0,)), ((), ())), preferred_element_type=jnp.float32)
            rounded = lax.optimization_barrier(partial_value.astype(jnp.bfloat16))
            return totals + rounded.astype(jnp.float32), None

        grads, unused = lax.scan(add_shard, jnp.zeros((FF, D), jnp.float32),
                                 (local_hidden.reshape(N_DP, N_EXPERT * CAP, FF), scaled.reshape(N_DP, N_EXPERT * CAP, D)))
        return grad_rows, grads, slot_scores

    grad_rows, grad_down, slot_scores = lax.map(expert_pass, (owners, filled, hidden, down_weight))
    grad_hidden = grad_rows.reshape(WINDOW, N_DP, N_EXPERT, CAP, FF)
    score_flat = jnp.concatenate([slot_scores.reshape(-1), jnp.zeros((1,), jnp.float32)])
    token_scores = score_flat[flat_place].reshape(TOKENS, TOPK)
    outside = jnp.where(chosen >= WINDOW, other_scores, jnp.float32(0.0))
    scores_all = jnp.where(live_slot, token_scores, outside)
    mean_score = jnp.sum(gating * scores_all, axis=1, keepdims=True)
    grad_logits = gating * (scores_all - mean_score)
    return grad_hidden, grad_down, grad_logits
```

```python
import functools

import jax
import jax.numpy as jnp
from jax import lax
from jax.experimental import pallas as pl
from jax.experimental.pallas import tpu as pltpu
from jax.sharding import PartitionSpec as P

MESH = pl.DeviceIdType.MESH
PIECES = 8
AHEAD = 3


def kernel(
    window, shards, capacity, pieces, ahead,
    token_hbm, logits_hbm, chosen_hbm, slots_hbm, other_hbm, hidden_hbm, weight_ref,
    gradh_ref, down_ref, logit_ref,
    token_ref, logits_ref, chosen_ref, slots_ref, other_ref, hidden_ref,
    rsend, rrecv, msend, mrecv, wfull, padded, hturn, upward, own, csend, crecv, ysend, yrecv,
    tsend, trecv, gates,
    rs, rr, ms, mr, ws, wr, dr, fs, cs, cr, ys, yr, ts, tr, ls, lw,
):
    me = lax.axis_index("expert")
    place = lax.axis_index("dp")
    chip, core = place // 2, place % 2
    chips = shards // 2
    mate = (me, chip * 2 + 1 - core)
    tokens, width = token_ref.shape
    piece = width // pieces
    rows = rsend.shape[2]
    slots_all = window * rows
    shard_rows, hidden_units = weight_ref.shape[0], hidden_ref.shape[2]

    def flipped(mask):
        where = me
        for bit in range(window.bit_length() - 1):
            if mask >> bit & 1:
                where = where + (1 << bit) * (1 - 2 * (me // (1 << bit) % 2))
        return where

    if window & (window - 1):
        near = [lax.rem(me + step, window) for step in range(window)]
    else:
        near = [flipped(mask) for mask in (0, *range(window - 1, 0, -1))]

    def other(step):
        return near[step]

    def settle(buffer, sem):
        whole = buffer.at[pl.ds(0, window - 1)]
        pltpu.make_async_copy(whole, whole, sem).wait()

    def chip_at(step):
        return lax.rem(chip + step, chips)

    def across(step):
        return (me, chip_at(step) * 2 + core)

    loads = [
        pltpu.make_async_copy(src, dst, ls.at[i])
        for i, (src, dst) in enumerate((
            (chosen_hbm, chosen_ref), (slots_hbm, slots_ref), (token_hbm, token_ref),
            (logits_hbm, logits_ref), (other_hbm, other_ref), (hidden_hbm, hidden_ref),
        ))
    ]
    for load in loads:
        load.start()
    keeps = [
        pltpu.make_async_copy(
            weight_ref.at[:, pl.ds(c * piece, piece)], wfull.at[c, place], lw
        )
        for c in range(pieces)
    ]

    def weight_copy(c, target, sem):
        lanes = pl.ds(pl.multiple_of(c * piece, piece), piece)
        return pltpu.make_async_remote_copy(
            src_ref=weight_ref.at[:, lanes], dst_ref=wfull.at[c, place],
            send_sem=ws, recv_sem=sem,
            device_id=target, device_id_type=MESH,
        )

    barrier = pltpu.get_barrier_semaphore()
    for step in range(1, window):
        pl.semaphore_signal(barrier, inc=1, device_id=(other(step), place), device_id_type=MESH)
    for step in range(1, chips):
        pl.semaphore_signal(barrier, inc=1, device_id=across(step), device_id_type=MESH)
    pl.semaphore_signal(barrier, inc=1, device_id=mate, device_id_type=MESH)

    k = logit_ref.shape[0]
    for load in loads[:5]:
        load.wait()
    raised = jnp.exp(logits_ref[...])
    gating = raised / jnp.sum(raised, axis=0, keepdims=True)
    sent_gate = gating.astype(jnp.bfloat16).astype(jnp.float32)
    chosen = chosen_ref[...]
    slots = slots_ref[...]
    outside = jnp.where(chosen >= window, other_ref[...], 0.0)
    live = slots < capacity
    for w in range(window):
        here = live & (chosen == w)
        pos = jnp.sum(jnp.where(here, slots.astype(jnp.float32) + 1.0, 0.0), axis=0, keepdims=True) - 1.0
        gate = jnp.sum(jnp.where(here, sent_gate, 0.0), axis=0, keepdims=True)
        line = lax.broadcasted_iota(jnp.int32, (8, tokens), 0)
        msend[w] = jnp.where(line == 0, pos, gate)

    slot_id = lax.broadcasted_iota(jnp.int32, (rows, tokens), 0).astype(jnp.float32)

    def spread(ref, w):
        return slot_id == ref[w, 0:1, :]

    dispatch = jnp.concatenate(
        [spread(msend, w).astype(jnp.float32) for w in range(window)], axis=0
    ).astype(jnp.bfloat16)

    def fill(c):
        lanes = pl.ds(pl.multiple_of(c * piece, piece), piece)
        placed = jnp.dot(dispatch, token_ref[:, lanes], preferred_element_type=jnp.float32)
        rsend[c] = placed.astype(jnp.bfloat16).reshape(window, rows, piece)

    def row_copy(c, dest, source):
        return pltpu.make_async_remote_copy(
            src_ref=rsend.at[c, dest, pl.ds(0, capacity)],
            dst_ref=rrecv.at[c, source, pl.ds(0, capacity)],
            send_sem=rs, recv_sem=rr.at[c],
            device_id=(dest, place), device_id_type=MESH,
        )

    def meta_copy(dest, source):
        return pltpu.make_async_remote_copy(
            src_ref=msend.at[dest], dst_ref=mrecv.at[source],
            send_sem=ms, recv_sem=mr,
            device_id=(dest, place), device_id_type=MESH,
        )

    def score_copy(dest, source):
        return pltpu.make_async_remote_copy(
            src_ref=tsend.at[dest], dst_ref=trecv.at[source],
            send_sem=ts, recv_sem=tr,
            device_id=(dest, place), device_id_type=MESH,
        )

    def pass_copy(c, slot):
        return pltpu.make_async_remote_copy(
            src_ref=wfull.at[c, slot], dst_ref=wfull.at[c, slot],
            send_sem=fs, recv_sem=dr.at[c],
            device_id=mate, device_id_type=MESH,
        )

    def core_copy(c):
        return pltpu.make_async_remote_copy(
            src_ref=csend.at[c], dst_ref=crecv.at[c],
            send_sem=cs, recv_sem=cr.at[c],
            device_id=mate, device_id_type=MESH,
        )

    def sum_copy(c, step):
        return pltpu.make_async_remote_copy(
            src_ref=ysend.at[c, step - 1], dst_ref=yrecv.at[c, step - 1],
            send_sem=ys, recv_sem=yr.at[c],
            device_id=across(step), device_id_type=MESH,
        )

    fill(0)
    pl.semaphore_wait(barrier, window - 1 + chips)

    def launch_weights(c, carry):
        for step in range(1, chips):
            weight_copy(c, across(step), wr.at[c, step - 1]).start()
        weight_copy(c, mate, dr.at[c]).start()
        return carry

    lax.fori_loop(0, pieces, launch_weights, 0)

    for step in range(1, window):
        meta_copy(other(step), me).start()

    def send_rows(c):
        for step in range(1, window):
            row_copy(c, other(step), me).start()

    def launch(c, carry):
        @pl.when(c < ahead)
        def _():
            send_rows(c)

        @pl.when(c + 1 < pieces)
        def _():
            fill(c + 1)

        return carry

    lax.fori_loop(0, pieces, launch, 0)

    mrecv[me] = msend[me]
    for c in range(pieces):
        rrecv[c, me, 0:capacity] = rsend[c, me, 0:capacity]
        if rows > capacity:
            rrecv[c, :, capacity:rows] = jnp.zeros((window, rows - capacity, piece), jnp.bfloat16)
        keeps[c].start()
    loads[5].wait()
    padded[:, 0:capacity] = hidden_ref[...]
    if rows > capacity:
        padded[:, capacity:rows] = jnp.zeros((window, rows - capacity, hidden_units), jnp.bfloat16)
    flat = padded[...].reshape(slots_all, hidden_units)
    hturn[...] = flat.T.reshape(shards, shard_rows, slots_all)
    upward[...] = jnp.zeros_like(upward)
    for keep in keeps:
        keep.wait()

    settle(mrecv, mr)
    for s in range(window):
        gates[s] = jnp.sum(
            jnp.where(spread(mrecv, s), mrecv[s, 1:2, :], 0.0), axis=1, keepdims=True
        )

    def combine(c):
        lanes = pl.ds(pl.multiple_of(c * piece, piece), piece)
        with jax.named_scope("w_core"):
            core_copy(c).wait_recv()
        for step in range(1, chips):
            to = chip_at(step)
            ysend[c, step - 1] = (own[c, to] + crecv[c, to].astype(jnp.float32)).astype(jnp.bfloat16)
            sum_copy(c, step).start()
        down_ref[:, lanes] = own[c, chip] + crecv[c, chip].astype(jnp.float32)

    def finish(c, carry):
        @pl.when(c > 0)
        def _():
            combine(c - 1)

        for step in range(1, chips):
            came = lax.rem(chip + chips - step, chips) * 2 + core
            weight_copy(c, mate, wr.at[c, step - 1]).wait_recv()
            pass_copy(c, came).start()
        came_rows = rrecv.at[c, pl.ds(0, window - 1), pl.ds(0, capacity)]
        with jax.named_scope("w_rows"):
            pltpu.make_async_copy(came_rows, came_rows, rr.at[c]).wait()

        @pl.when(c + ahead < pieces)
        def _():
            send_rows(c + ahead)

        got = rrecv[c].reshape(slots_all, piece)
        scaled = (gates[...].reshape(slots_all, 1) * got.astype(jnp.float32)).astype(jnp.bfloat16)
        for h in range(chips):
            csend[c, h] = jnp.dot(
                hturn[2 * h + 1 - core], scaled, preferred_element_type=jnp.float32
            ).astype(jnp.bfloat16)
        core_copy(c).start()
        for h in range(chips):
            own[c, h] = jnp.dot(hturn[2 * h + core], scaled, preferred_element_type=jnp.float32)
        with jax.named_scope("w_mate"):
            from_mate = wfull.at[c, pl.ds(0, chips)]
            pltpu.make_async_copy(from_mate, from_mate, dr.at[c]).wait()
        weights = wfull[c].reshape(hidden_units, piece)
        upward[...] += lax.dot_general(
            got, weights, (((1,), (1,)), ((), ())), preferred_element_type=jnp.float32
        )
        return carry

    lax.fori_loop(0, pieces, finish, 0)
    combine(pieces - 1)

    for s in range(window):
        up = upward[s * rows : (s + 1) * rows]
        score = jnp.sum(padded[s].astype(jnp.float32) * up, axis=1, keepdims=True)
        back = jnp.sum(jnp.where(spread(mrecv, s), score, 0.0), axis=0, keepdims=True)
        tsend[s] = jnp.broadcast_to(back, (8, tokens))
    for step in range(1, window):
        score_copy(other(step), me).start()
    trecv[me] = tsend[me]
    for s in range(window):
        up = upward[s * rows : s * rows + capacity]
        gradh_ref[s] = (gates[s, 0:capacity] * up).astype(jnp.bfloat16)

    def collect(c, carry):
        lanes = pl.ds(pl.multiple_of(c * piece, piece), piece)
        with jax.named_scope("w_sum"):
            came = yrecv.at[c]
            pltpu.make_async_copy(came, came, yr.at[c]).wait()
        for step in range(1, chips):
            down_ref[:, lanes] += yrecv[c, step - 1].astype(jnp.float32)
        return carry

    def sent(whole, sem):
        pltpu.make_async_copy(whole, whole, sem).wait()

    sent(wfull.at[:, pl.ds(0, chips)], ws)
    sent(wfull.at[:, pl.ds(0, chips - 1)], fs)
    sent(csend, cs)
    sent(rsend.at[:, pl.ds(0, window - 1), pl.ds(0, capacity)], rs)
    settle(msend, ms)
    lax.fori_loop(0, pieces - 1, collect, 0)

    settle(trecv, tr)
    token_scores = jnp.zeros((k, tokens), jnp.float32)
    for w in range(window):
        token_scores = jnp.where(chosen == w, trecv[w], token_scores)
    scores_all = jnp.where(live, token_scores, outside)
    mean_score = jnp.sum(gating * scores_all, axis=0, keepdims=True)
    logit_ref[...] = gating * (scores_all - mean_score)
    settle(tsend, ts)

    collect(pieces - 1, 0)
    sent(ysend, ys)


def write_out(a, b, c, a_out, b_out, c_out, sems):
    copies = [
        pltpu.make_async_copy(src, dst, sems.at[i])
        for i, (src, dst) in enumerate(((b, b_out), (a, a_out), (c, c_out)))
    ]
    for copy in copies:
        copy.start()
    for copy in copies:
        copy.wait()


def fused(grad_output, logits, chosen, slots, other_scores, hidden, down_weight):
    window = lax.axis_size("expert")
    shards = lax.axis_size("dp")
    capacity, hidden_units = hidden.shape[3], hidden.shape[4]
    tokens, width = grad_output.shape
    k = logits.shape[1]
    shard_rows = down_weight.shape[1]
    rows = -(-capacity // 16) * 16
    chips = shards // 2
    piece = width // PIECES
    vmem = pl.BlockSpec(memory_space=pltpu.VMEM)
    hbm = pl.BlockSpec(memory_space=pltpu.HBM)
    bf, f32, dma = jnp.bfloat16, jnp.float32, pltpu.SemaphoreType.DMA
    slots_all = window * rows
    gradh, down, turned = pl.pallas_call(
        functools.partial(kernel, window, shards, capacity, PIECES, min(AHEAD, PIECES)),
        out_shape=(
            jax.ShapeDtypeStruct((window, capacity, hidden_units), bf),
            jax.ShapeDtypeStruct((shard_rows, width), f32),
            jax.ShapeDtypeStruct((k, tokens), f32),
        ),
        in_specs=[hbm] * 7,
        out_specs=(vmem,) * 3,
        scratch_shapes=[
            pltpu.VMEM((tokens, width), bf),
            pltpu.VMEM((k, tokens), f32),
            pltpu.VMEM((k, tokens), jnp.int32),
            pltpu.VMEM((k, tokens), jnp.int32),
            pltpu.VMEM((k, tokens), f32),
            pltpu.VMEM((window, capacity, hidden_units), bf),
            pltpu.VMEM((PIECES, window, rows, piece), bf),
            pltpu.VMEM((PIECES, window, rows, piece), bf),
            pltpu.VMEM((window, 8, tokens), f32),
            pltpu.VMEM((window, 8, tokens), f32),
            pltpu.VMEM((PIECES, shards, shard_rows, piece), bf),
            pltpu.VMEM((window, rows, hidden_units), bf),
            pltpu.VMEM((shards, shard_rows, slots_all), bf),
            pltpu.VMEM((slots_all, hidden_units), f32),
            pltpu.VMEM((PIECES, chips, shard_rows, piece), f32),
            pltpu.VMEM((PIECES, chips, shard_rows, piece), bf),
            pltpu.VMEM((PIECES, chips, shard_rows, piece), bf),
            pltpu.VMEM((PIECES, chips - 1, shard_rows, piece), bf),
            pltpu.VMEM((PIECES, chips - 1, shard_rows, piece), bf),
            pltpu.VMEM((window, 8, tokens), f32),
            pltpu.VMEM((window, 8, tokens), f32),
            pltpu.VMEM((window, rows, 1), f32),
            dma, dma((PIECES,)),
            dma, dma,
            dma, dma((PIECES, chips - 1)), dma((PIECES,)),
            dma,
            dma, dma((PIECES,)),
            dma, dma((PIECES,)),
            dma, dma,
            dma((6,)), dma,
        ],
        compiler_params=pltpu.CompilerParams(
            collective_id=0, has_side_effects=True, vmem_limit_bytes=48 * 1024 * 1024
        ),
    )(*(pltpu.with_memory_space_constraint(a, pltpu.HBM) for a in (
        grad_output, logits.T, chosen.T, slots.T, other_scores.T,
        hidden.reshape(window, capacity, hidden_units), down_weight.reshape(shard_rows, width),
    )))
    gradh, down, turned = (
        pltpu.with_memory_space_constraint(a, pltpu.VMEM) for a in (gradh, down, turned)
    )
    gradh, down, turned = pl.pallas_call(
        write_out,
        out_shape=tuple(jax.ShapeDtypeStruct(a.shape, a.dtype) for a in (gradh, down, turned)),
        in_specs=[vmem] * 3,
        out_specs=(hbm,) * 3,
        scratch_shapes=[dma((3,))],
        compiler_params=pltpu.CompilerParams(vmem_limit_bytes=8 * 1024 * 1024),
    )(gradh, down, turned)
    return (gradh.reshape(hidden.shape), down.reshape(1, shard_rows, width), turned.T)


def plain(grad_output, logits, chosen, slots, other_scores, hidden, down_weight):
    window = lax.axis_size("expert")
    capacity = hidden.shape[3]
    hidden_units = hidden.shape[4]
    model_width = grad_output.shape[1]
    shard_rows = down_weight.shape[1]
    raised = jnp.exp(logits)
    gating = raised / jnp.sum(raised, axis=1, keepdims=True)
    gate_sent = gating.astype(jnp.bfloat16)
    live_slot = slots < capacity
    target = jnp.where(live_slot, chosen * capacity + slots, window * capacity)
    columns = jnp.arange(window * capacity, dtype=jnp.int32)
    placing = (target[:, :, None] == columns[None, None, :]).astype(jnp.bfloat16)
    dispatch = jnp.sum(placing, axis=1)
    send_rows = jnp.einsum(
        "tr,td->rd", dispatch, grad_output, preferred_element_type=jnp.float32
    ).astype(jnp.bfloat16)
    send_gate = jnp.einsum(
        "tkr,tk->r", placing, gate_sent, preferred_element_type=jnp.float32
    ).astype(jnp.bfloat16)
    placing_float = placing.astype(jnp.float32)
    send_rows = send_rows.reshape(window, capacity, model_width)
    send_gate = send_gate.reshape(window, capacity)
    recv_rows, recv_gate = (
        lax.all_to_all(send_rows, "expert", split_axis=0, concat_axis=0, tiled=True),
        lax.all_to_all(send_gate, "expert", split_axis=0, concat_axis=0, tiled=True),
    )
    slot_rows = recv_rows.reshape(-1, model_width)
    slot_gate = recv_gate.reshape(-1).astype(jnp.float32)
    local_hidden = hidden.reshape(-1, hidden_units)
    scaled = (slot_gate[:, None] * slot_rows.astype(jnp.float32)).astype(jnp.bfloat16)
    weights = down_weight.reshape(shard_rows, model_width)
    product = lax.dot_general(
        slot_rows,
        lax.all_gather(weights, "dp", axis=0, tiled=True),
        (((1,), (1,)), ((), ())),
        preferred_element_type=jnp.float32,
    )
    grad_rows = lax.psum_scatter(
        lax.dot_general(
            local_hidden, scaled, (((0,), (0,)), ((), ())), preferred_element_type=jnp.float32
        ).astype(jnp.bfloat16),
        "dp",
        scatter_dimension=0,
        tiled=True,
    ).astype(jnp.float32)
    slot_scores = jnp.sum(local_hidden.astype(jnp.float32) * product, axis=1)
    grad_hidden = (slot_gate[:, None] * product).astype(jnp.bfloat16).reshape(hidden.shape)
    returned = lax.all_to_all(
        slot_scores.reshape(window, capacity), "expert", split_axis=0, concat_axis=0, tiled=True
    )
    token_scores = jnp.einsum(
        "tkr,r->tk", placing_float, returned.reshape(-1), precision=lax.Precision.HIGHEST
    )
    outside = jnp.where(chosen >= window, other_scores, jnp.float32(0.0))
    scores_all = jnp.where(live_slot, token_scores, outside)
    mean_score = jnp.sum(gating * scores_all, axis=1, keepdims=True)
    grad_logits = gating * (scores_all - mean_score)
    return (grad_hidden, grad_rows.reshape(1, shard_rows, model_width), grad_logits)


def body(grad_output, logits, chosen, slots, other_scores, hidden, down_weight):
    args = (grad_output, logits, chosen, slots, other_scores, hidden, down_weight)
    fits = (
        lax.axis_size("dp") % 2 == 0
        and lax.axis_size("dp") > 2
        and hidden.shape[3] % 8 == 0
        and down_weight.shape[1] % 16 == 0
        and hidden.shape[4] % 128 == 0
        and grad_output.shape[0] == 128
        and grad_output.shape[1] % (PIECES * 128) == 0
        and logits.shape[1] == 8
    )
    return fused(*args) if fits else plain(*args)


def solution(mesh):
    placed = (
        P(("expert", "dp"), None),
        P(("expert", "dp"), None),
        P(("expert", "dp"), None),
        P(("expert", "dp"), None),
        P(("expert", "dp"), None),
        P("expert", "dp", None, None, None),
        P("expert", "dp", None),
    )
    return jax.shard_map(
        body,
        mesh=mesh,
        in_specs=placed,
        out_specs=(
            P("expert", "dp", None, None, None),
            P("expert", "dp", None),
            P(("expert", "dp"), None),
        ),
        check_vma=False,
    )
```

```python
import functools

import jax
import jax.numpy as jnp
from jax import lax
from jax.experimental import pallas as pl
from jax.experimental.pallas import tpu as pltpu
from jax.sharding import PartitionSpec as P

MESH = pl.DeviceIdType.MESH
PIECES = 8
FIRST = 0
LAST = 0
AHEAD = 2
NEAR_AHEAD = 4
DIRECT_AHEAD = 3
COLUMNS = 2


def kernel(
    window, shards, capacity, pieces, first, last, ahead, near_ahead, direct_ahead, columns,
    token_hbm, logits_hbm, chosen_hbm, slots_hbm, other_hbm, hidden_hbm, weight_ref,
    gradh_ref, down_ref, logit_ref,
    token_ref, logits_ref, chosen_ref, slots_ref, other_ref, hidden_ref,
    rsend, rrecv, msend, mrecv, wfull, padded, hturn, upward, own, csend, crecv, ysend, yrecv,
    tsend, trecv, gates, tin, fsend, lsend, fmeta, fplace, lplace,
    rs, rr, ms, mr, ws, wr, dr, fs, cs, cr, ys, yr, ts, tr, ls, lw, go,
    rf, ro, bs, br, bo, ps, pm, qs, qr,
):
    me = lax.axis_index("expert")
    place = lax.axis_index("dp")
    chip, core = place // 2, place % 2
    chips = shards // 2
    mate = (me, chip * 2 + 1 - core)
    tokens, width = token_ref.shape
    piece = width // pieces
    rows = rsend.shape[2]
    slots_all = window * rows
    shard_rows, hidden_units = weight_ref.shape[0], hidden_ref.shape[2]

    def flipped(mask):
        where = me
        for bit in range(window.bit_length() - 1):
            if mask >> bit & 1:
                where = where + (1 << bit) * (1 - 2 * (me // (1 << bit) % 2))
        return where

    near = [flipped(mask) for mask in (0, *range(window - 1, 0, -1))]

    level, column = me // columns, me % columns
    half, members = level // 2, window // 2
    base, far_base = half * members, (1 - half) * members
    inner = (level + 1) // 2 % 2
    side = level % 2
    own_level = side * columns
    beyond = (2 - half) * columns + column
    inward = (1 + half) * columns + column
    outward = half * 3 * columns + column
    far_dests = [flipped(mask) for mask in range(window - 1, members - 1, -1)]
    near_dests = [flipped(mask) for mask in range(members - 1, 0, -1)]
    off_level = [flipped(mask) for mask in range(members - 1, columns - 1, -1)]
    beside = [flipped(mask) for mask in range(columns - 1, 0, -1)]

    relayed = pieces - first - last
    end = first + relayed

    def is_relayed(c):
        return (c >= first) & (c < end)

    def other(step):
        return near[step]

    def settle(buffer, sem):
        whole = buffer.at[pl.ds(0, window - 1)]
        pltpu.make_async_copy(whole, whole, sem).wait()

    def chip_at(step):
        return lax.rem(chip + step, chips)

    def across(step):
        return (me, chip_at(step) * 2 + core)

    loads = [
        pltpu.make_async_copy(src, dst, ls.at[i])
        for i, (src, dst) in enumerate((
            (chosen_hbm, chosen_ref), (slots_hbm, slots_ref), (token_hbm, token_ref),
            (logits_hbm, logits_ref), (other_hbm, other_ref), (hidden_hbm, hidden_ref),
        ))
    ]
    for load in loads:
        load.start()
    keeps = [
        pltpu.make_async_copy(
            weight_ref.at[:, pl.ds(c * piece, piece)], wfull.at[c, place], lw
        )
        for c in range(pieces)
    ]

    def weight_copy(c, target, sem):
        lanes = pl.ds(pl.multiple_of(c * piece, piece), piece)
        return pltpu.make_async_remote_copy(
            src_ref=weight_ref.at[:, lanes], dst_ref=wfull.at[c, place],
            send_sem=ws, recv_sem=sem,
            device_id=target, device_id_type=MESH,
        )

    barrier = pltpu.get_barrier_semaphore()

    def signal(sem, target):
        pl.semaphore_signal(sem, inc=1, device_id=target, device_id_type=MESH)

    for step in range(1, chips):
        signal(barrier, (me, chip_at(step) * 2 + 1))

    @pl.when(core == 0)
    def _():
        signal(barrier, mate)

    for step in range(1, window):
        signal(barrier, (other(step), chip * 2))

    @pl.when(core == 1)
    def _():
        with jax.named_scope("w_near"):
            pl.semaphore_wait(barrier, 2 * chips - 1)
        signal(go, mate)

    @pl.when(core == 0)
    def _():
        with jax.named_scope("w_near"):
            pl.semaphore_wait(go, 1)

    def launch_weights(c, carry):
        for step in range(1, chips):
            weight_copy(c, across(step), wr.at[c, step - 1]).start()
        weight_copy(c, mate, dr.at[c]).start()
        return carry

    lax.fori_loop(0, pieces, launch_weights, 0)

    k = logit_ref.shape[0]
    for load in loads[:5]:
        load.wait()
    raised = jnp.exp(logits_ref[...])
    gating = raised / jnp.sum(raised, axis=0, keepdims=True)
    sent_gate = gating.astype(jnp.bfloat16).astype(jnp.float32)
    chosen = chosen_ref[...]
    slots = slots_ref[...]
    outside = jnp.where(chosen >= window, other_ref[...], 0.0)
    live = slots < capacity
    for w in range(window):
        here = live & (chosen == w)
        pos = jnp.sum(jnp.where(here, slots.astype(jnp.float32) + 1.0, 0.0), axis=0, keepdims=True) - 1.0
        gate = jnp.sum(jnp.where(here, sent_gate, 0.0), axis=0, keepdims=True)
        line = lax.broadcasted_iota(jnp.int32, (2, tokens), 0)
        msend[w] = jnp.where(line == 0, pos, gate)

    slot_id = lax.broadcasted_iota(jnp.int32, (rows, tokens), 0).astype(jnp.float32)

    def spread(ref, w):
        return slot_id == ref[w, 0:1, :]

    def placing(first):
        return jnp.concatenate(
            [spread(msend, first + w).astype(jnp.float32) for w in range(members)], axis=0
        ).astype(jnp.bfloat16)

    dispatch, far_dispatch = placing(base), placing(far_base)

    def fill(c, matrix, first):
        lanes = pl.ds(pl.multiple_of(c * piece, piece), piece)
        placed = jnp.dot(matrix, token_ref[:, lanes], preferred_element_type=jnp.float32)
        rsend[c, pl.ds(first, members)] = placed.astype(jnp.bfloat16).reshape(members, rows, piece)

    def block_copy(c, dest, slot, sem):
        lanes = pl.ds(pl.multiple_of(c * piece, piece), piece)
        return pltpu.make_async_remote_copy(
            src_ref=token_ref.at[:, lanes], dst_ref=tin.at[c - first, slot],
            send_sem=bs, recv_sem=sem.at[c - first],
            device_id=(dest, place), device_id_type=MESH,
        )

    def pass_block(c):
        return pltpu.make_async_remote_copy(
            src_ref=tin.at[c - first, 2], dst_ref=tin.at[c - first, 1 - side],
            send_sem=bs, recv_sem=br.at[c - first],
            device_id=(beyond, place), device_id_type=MESH,
        )

    def far_meta(first, dest, slot):
        return pltpu.make_async_remote_copy(
            src_ref=msend.at[pl.ds(first, members)], dst_ref=fmeta.at[slot],
            send_sem=qs, recv_sem=qr,
            device_id=(dest, place), device_id_type=MESH,
        )

    def forward_copy(block, c, source, dest, sem):
        return pltpu.make_async_remote_copy(
            src_ref=block.at[pl.ds(0, capacity)],
            dst_ref=rrecv.at[c, source, pl.ds(0, capacity)],
            send_sem=sem, recv_sem=rr.at[c],
            device_id=(dest, place), device_id_type=MESH,
        )

    def row_copy(c, dest, source, sem):
        return pltpu.make_async_remote_copy(
            src_ref=rsend.at[c, dest, pl.ds(0, capacity)],
            dst_ref=rrecv.at[c, source, pl.ds(0, capacity)],
            send_sem=sem, recv_sem=rr.at[c],
            device_id=(dest, place), device_id_type=MESH,
        )

    def meta_copy(dest, source):
        return pltpu.make_async_remote_copy(
            src_ref=msend.at[dest], dst_ref=mrecv.at[source],
            send_sem=ms, recv_sem=mr,
            device_id=(dest, place), device_id_type=MESH,
        )

    def score_copy(dest, source):
        return pltpu.make_async_remote_copy(
            src_ref=tsend.at[dest], dst_ref=trecv.at[source],
            send_sem=ts, recv_sem=tr,
            device_id=(dest, place), device_id_type=MESH,
        )

    def pass_copy(c, slot):
        return pltpu.make_async_remote_copy(
            src_ref=wfull.at[c, slot], dst_ref=wfull.at[c, slot],
            send_sem=fs, recv_sem=dr.at[c],
            device_id=mate, device_id_type=MESH,
        )

    def core_copy(c):
        return pltpu.make_async_remote_copy(
            src_ref=csend.at[c], dst_ref=crecv.at[c],
            send_sem=cs, recv_sem=cr.at[c],
            device_id=mate, device_id_type=MESH,
        )

    def sum_copy(c, step):
        return pltpu.make_async_remote_copy(
            src_ref=ysend.at[c, step - 1], dst_ref=yrecv.at[c, step - 1],
            send_sem=ys, recv_sem=yr.at[c],
            device_id=across(step), device_id_type=MESH,
        )

    fill(0, dispatch, base)
    for c in range(first):
        fill(c, far_dispatch, far_base)

    @pl.when(core == 0)
    def _():
        with jax.named_scope("w_bar"):
            pl.semaphore_wait(barrier, 2 * (window - 1))
        signal(go, mate)

    @pl.when(core == 1)
    def _():
        with jax.named_scope("w_bar"):
            pl.semaphore_wait(go, 1)


    @pl.when(inner == 1)
    def _():
        far_meta(far_base, beyond, side).start()

    @pl.when(inner == 0)
    def _():
        far_meta(far_base, beyond, side).start()
        far_meta(base, inward, 2).start()

    for step in range(1, window):
        meta_copy(other(step), me).start()

    def send_near(c):
        for dest in beside:
            row_copy(c, dest, me, rs).start()

        @pl.when((inner == 1) | jnp.logical_not(is_relayed(c)))
        def _():
            for dest in off_level:
                row_copy(c, dest, me, ro).start()

    def send_far(c):
        for dest in far_dests:
            row_copy(c, dest, me, rf).start()

    for c in range(first):
        send_far(c)
        send_near(c)

    @pl.when(inner == 1)
    def _():
        for c in range(first, first + ahead):
            block_copy(c, beyond, side, br).start()

    @pl.when(inner == 0)
    def _():
        for c in range(first, end):
            block_copy(c, inward, 2, bo).start()

    def launch(c, carry):
        @pl.when((c >= first) & ((inner == 0) & (c < end) | (inner == 1) & (c < first + near_ahead)))
        def _():
            send_near(c)

        @pl.when(c + 1 < pieces)
        def _():
            fill(c + 1, dispatch, base)

        return carry

    lax.fori_loop(0, pieces, launch, 0)
    for c in range(end, pieces):
        fill(c, far_dispatch, far_base)

    mrecv[me] = msend[me]
    for c in range(pieces):
        rrecv[c, me, 0:capacity] = rsend[c, me, 0:capacity]
        if rows > capacity:
            rrecv[c, :, capacity:rows] = jnp.zeros((window, rows - capacity, piece), jnp.bfloat16)
        keeps[c].start()
    loads[5].wait()
    padded[:, 0:capacity] = hidden_ref[...]
    if rows > capacity:
        padded[:, capacity:rows] = jnp.zeros((window, rows - capacity, hidden_units), jnp.bfloat16)
    flat = padded[...].reshape(slots_all, hidden_units)
    hturn[...] = flat.T.reshape(shards, shard_rows, slots_all)
    upward[...] = jnp.zeros_like(upward)
    for keep in keeps:
        keep.wait()

    settle(mrecv, mr)
    for s in range(window):
        gates[s] = jnp.sum(
            jnp.where(spread(mrecv, s), mrecv[s, 1:2, :], 0.0), axis=1, keepdims=True
        )

    def pump(c):
        with jax.named_scope("w_pump"):
            block = tin.at[c - first, 2]
            pltpu.make_async_copy(block, block, bo.at[c - first]).wait()
        pass_block(c).start()

    def relay(c):
        with jax.named_scope("w_relay"):
            blocks = tin.at[c - first, pl.ds(0, 2)]
            pltpu.make_async_copy(blocks, blocks, br.at[c - first]).wait()

        @pl.when(c + ahead < end)
        def _():
            block_copy(c + ahead, beyond, side, br).start()
            pump(c + ahead)

        if last:
            @pl.when((c + ahead >= end) & (c + ahead < pieces))
            def _():
                send_far(c + ahead)

        sources = [((1 - half) * 2 + i) * columns + column for i in range(2)]
        for i in range(2):
            placed = jnp.dot(fplace[i], tin[c - first, i], preferred_element_type=jnp.float32)
            fsend[c - first, i] = placed.astype(jnp.bfloat16).reshape(members, rows, piece)
        placed = jnp.dot(lplace[...], tin[c - first, 2], preferred_element_type=jnp.float32)
        lsend[c - first] = placed.astype(jnp.bfloat16).reshape(columns, rows, piece)
        for dest in near_dests:
            for i in range(2):
                forward_copy(fsend.at[c - first, i, dest - base], c, sources[i], dest, ps).start()
        for dest in beside:
            forward_copy(lsend.at[c - first, dest % columns], c, outward, dest, pm).start()

        @pl.when(c + near_ahead < pieces)
        def _():
            send_near(c + near_ahead)

        for i in range(2):
            rrecv[c, sources[i], 0:capacity] = fsend[c - first, i, me - base, 0:capacity]
        rrecv[c, outward, 0:capacity] = lsend[c - first, column, 0:capacity]

    @pl.when(inner == 1)
    def _():
        pltpu.make_async_copy(fmeta, fmeta, qr).wait()
        for i in range(2):
            fplace[i] = jnp.concatenate(
                [(slot_id == fmeta[i, w, 0:1, :]).astype(jnp.float32) for w in range(members)], axis=0
            ).astype(jnp.bfloat16)
        lplace[...] = jnp.concatenate(
            [
                (slot_id == fmeta[2, own_level + w, 0:1, :]).astype(jnp.float32)
                for w in range(columns)
            ],
            axis=0,
        ).astype(jnp.bfloat16)
        for c in range(first, first + ahead):
            pump(c)
        relay(first)

    def combine(c):
        lanes = pl.ds(pl.multiple_of(c * piece, piece), piece)
        with jax.named_scope("w_core"):
            core_copy(c).wait_recv()
        for step in range(1, chips):
            to = chip_at(step)
            ysend[c, step - 1] = (own[c, to] + crecv[c, to].astype(jnp.float32)).astype(jnp.bfloat16)
            sum_copy(c, step).start()
        down_ref[:, lanes] = own[c, chip] + crecv[c, chip].astype(jnp.float32)

    def finish(c, carry):
        @pl.when((inner == 1) & (c + 1 > first) & (c + 1 < end))
        def _():
            relay(c + 1)

        @pl.when(c > 0)
        def _():
            combine(c - 1)

        for step in range(1, chips):
            came = lax.rem(chip + chips - step, chips) * 2 + core
            weight_copy(c, mate, wr.at[c, step - 1]).wait_recv()
            pass_copy(c, came).start()
        def rows_in(count):
            came_rows = rrecv.at[c, pl.ds(0, count), pl.ds(0, capacity)]
            with jax.named_scope("w_rows"):
                pltpu.make_async_copy(came_rows, came_rows, rr.at[c]).wait()

        kept = (inner == 1) & is_relayed(c)

        @pl.when(kept)
        def _():
            rows_in(window - 4)

        @pl.when(jnp.logical_not(kept))
        def _():
            rows_in(window - 1)

        if last:
            later = c + direct_ahead

            @pl.when((inner == 0) & (later >= end) & (later < pieces))
            def _():
                send_far(later)
                send_near(later)

        got = rrecv[c].reshape(slots_all, piece)
        scaled = (gates[...].reshape(slots_all, 1) * got.astype(jnp.float32)).astype(jnp.bfloat16)
        for h in range(chips):
            csend[c, h] = jnp.dot(
                hturn[2 * h + 1 - core], scaled, preferred_element_type=jnp.float32
            ).astype(jnp.bfloat16)
        core_copy(c).start()
        for h in range(chips):
            own[c, h] = jnp.dot(hturn[2 * h + core], scaled, preferred_element_type=jnp.float32)
        with jax.named_scope("w_mate"):
            from_mate = wfull.at[c, pl.ds(0, chips)]
            pltpu.make_async_copy(from_mate, from_mate, dr.at[c]).wait()
        weights = wfull[c].reshape(hidden_units, piece)
        upward[...] += lax.dot_general(
            got, weights, (((1,), (1,)), ((), ())), preferred_element_type=jnp.float32
        )
        return carry

    lax.fori_loop(0, pieces, finish, 0)
    combine(pieces - 1)

    for s in range(window):
        up = upward[s * rows : (s + 1) * rows]
        score = jnp.sum(padded[s].astype(jnp.float32) * up, axis=1, keepdims=True)
        back = jnp.sum(jnp.where(spread(mrecv, s), score, 0.0), axis=0, keepdims=True)
        tsend[s] = back
    for step in range(1, window):
        score_copy(other(step), me).start()
    trecv[me] = tsend[me]
    for s in range(window):
        up = upward[s * rows : s * rows + capacity]
        gradh_ref[s] = (gates[s, 0:capacity] * up).astype(jnp.bfloat16)

    def collect(c, carry):
        lanes = pl.ds(pl.multiple_of(c * piece, piece), piece)
        with jax.named_scope("w_sum"):
            came = yrecv.at[c]
            pltpu.make_async_copy(came, came, yr.at[c]).wait()
        for step in range(1, chips):
            down_ref[:, lanes] += yrecv[c, step - 1].astype(jnp.float32)
        return carry

    def sent(whole, sem):
        pltpu.make_async_copy(whole, whole, sem).wait()

    sent(wfull.at[:, pl.ds(0, chips)], ws)
    sent(wfull.at[:, pl.ds(0, chips - 1)], fs)
    sent(csend, cs)
    direct = first + last
    sent(rsend.at[:, pl.ds(0, columns - 1), pl.ds(0, capacity)], rs)
    if direct:
        sent(rsend.at[pl.ds(0, direct), pl.ds(0, members), pl.ds(0, capacity)], rf)

    @pl.when(inner == 1)
    def _():
        sent(rsend.at[:, pl.ds(0, members - columns), pl.ds(0, capacity)], ro)
        sent(tin.at[:, pl.ds(0, 2)], bs)
        sent(msend.at[pl.ds(0, members)], qs)
        sent(fsend.at[:, :, pl.ds(0, members - 1), pl.ds(0, capacity)], ps)
        sent(lsend.at[:, pl.ds(0, columns - 1), pl.ds(0, capacity)], pm)

    @pl.when(inner == 0)
    def _():
        if direct:
            sent(rsend.at[pl.ds(0, direct), pl.ds(0, members - columns), pl.ds(0, capacity)], ro)
        sent(tin.at[:, 0], bs)
        sent(msend, qs)

    settle(msend, ms)
    lax.fori_loop(0, pieces - 1, collect, 0)

    settle(trecv, tr)
    token_scores = jnp.zeros((k, tokens), jnp.float32)
    for w in range(window):
        token_scores = jnp.where(chosen == w, trecv[w], token_scores)
    scores_all = jnp.where(live, token_scores, outside)
    mean_score = jnp.sum(gating * scores_all, axis=0, keepdims=True)
    logit_ref[...] = gating * (scores_all - mean_score)
    settle(tsend, ts)

    collect(pieces - 1, 0)
    sent(ysend, ys)


def write_out(a, b, c, a_out, b_out, c_out, sems):
    copies = [
        pltpu.make_async_copy(src, dst, sems.at[i])
        for i, (src, dst) in enumerate(((b, b_out), (a, a_out), (c, c_out)))
    ]
    for copy in copies:
        copy.start()
    for copy in copies:
        copy.wait()


def fused(grad_output, logits, chosen, slots, other_scores, hidden, down_weight):
    window = lax.axis_size("expert")
    shards = lax.axis_size("dp")
    capacity, hidden_units = hidden.shape[3], hidden.shape[4]
    tokens, width = grad_output.shape
    k = logits.shape[1]
    shard_rows = down_weight.shape[1]
    rows = -(-capacity // 16) * 16
    chips = shards // 2
    piece = width // PIECES
    vmem = pl.BlockSpec(memory_space=pltpu.VMEM)
    hbm = pl.BlockSpec(memory_space=pltpu.HBM)
    bf, f32, dma = jnp.bfloat16, jnp.float32, pltpu.SemaphoreType.DMA
    slots_all = window * rows
    gradh, down, turned = pl.pallas_call(
        functools.partial(
            kernel, window, shards, capacity, PIECES, FIRST, LAST, AHEAD, NEAR_AHEAD, DIRECT_AHEAD,
            COLUMNS,
        ),
        out_shape=(
            jax.ShapeDtypeStruct((window, capacity, hidden_units), bf),
            jax.ShapeDtypeStruct((shard_rows, width), f32),
            jax.ShapeDtypeStruct((k, tokens), f32),
        ),
        in_specs=[hbm] * 7,
        out_specs=(vmem,) * 3,
        scratch_shapes=[
            pltpu.VMEM((tokens, width), bf),
            pltpu.VMEM((k, tokens), f32),
            pltpu.VMEM((k, tokens), jnp.int32),
            pltpu.VMEM((k, tokens), jnp.int32),
            pltpu.VMEM((k, tokens), f32),
            pltpu.VMEM((window, capacity, hidden_units), bf),
            pltpu.VMEM((PIECES, window, rows, piece), bf),
            pltpu.VMEM((PIECES, window, rows, piece), bf),
            pltpu.VMEM((window, 2, tokens), f32),
            pltpu.VMEM((window, 2, tokens), f32),
            pltpu.VMEM((PIECES, shards, shard_rows, piece), bf),
            pltpu.VMEM((window, rows, hidden_units), bf),
            pltpu.VMEM((shards, shard_rows, slots_all), bf),
            pltpu.VMEM((slots_all, hidden_units), f32),
            pltpu.VMEM((PIECES, chips, shard_rows, piece), f32),
            pltpu.VMEM((PIECES, chips, shard_rows, piece), bf),
            pltpu.VMEM((PIECES, chips, shard_rows, piece), bf),
            pltpu.VMEM((PIECES, chips - 1, shard_rows, piece), bf),
            pltpu.VMEM((PIECES, chips - 1, shard_rows, piece), bf),
            pltpu.VMEM((window, 1, tokens), f32),
            pltpu.VMEM((window, 1, tokens), f32),
            pltpu.VMEM((window, rows, 1), f32),
            pltpu.VMEM((PIECES - FIRST - LAST, 3, tokens, piece), bf),
            pltpu.VMEM((PIECES - FIRST - LAST, 2, window // 2, rows, piece), bf),
            pltpu.VMEM((PIECES - FIRST - LAST, COLUMNS, rows, piece), bf),
            pltpu.VMEM((3, window // 2, 2, tokens), f32),
            pltpu.VMEM((2, window // 2 * rows, tokens), bf),
            pltpu.VMEM((COLUMNS * rows, tokens), bf),
            dma, dma((PIECES,)),
            dma, dma,
            dma, dma((PIECES, chips - 1)), dma((PIECES,)),
            dma,
            dma, dma((PIECES,)),
            dma, dma((PIECES,)),
            dma, dma,
            dma((6,)), dma, pltpu.SemaphoreType.REGULAR,
            dma, dma, dma, dma((PIECES - FIRST - LAST,)), dma((PIECES - FIRST - LAST,)), dma, dma, dma, dma,
        ],
        compiler_params=pltpu.CompilerParams(
            collective_id=0, has_side_effects=True, vmem_limit_bytes=48 * 1024 * 1024
        ),
    )(*(pltpu.with_memory_space_constraint(a, pltpu.HBM) for a in (
        grad_output, logits.T, chosen.T, slots.T, other_scores.T,
        hidden.reshape(window, capacity, hidden_units), down_weight.reshape(shard_rows, width),
    )))
    gradh, down, turned = (
        pltpu.with_memory_space_constraint(a, pltpu.VMEM) for a in (gradh, down, turned)
    )
    gradh, down, turned = pl.pallas_call(
        write_out,
        out_shape=tuple(jax.ShapeDtypeStruct(a.shape, a.dtype) for a in (gradh, down, turned)),
        in_specs=[vmem] * 3,
        out_specs=(hbm,) * 3,
        scratch_shapes=[dma((3,))],
        compiler_params=pltpu.CompilerParams(vmem_limit_bytes=8 * 1024 * 1024),
    )(gradh, down, turned)
    return (gradh.reshape(hidden.shape), down.reshape(1, shard_rows, width), turned.T)


def plain(grad_output, logits, chosen, slots, other_scores, hidden, down_weight):
    window = lax.axis_size("expert")
    capacity = hidden.shape[3]
    hidden_units = hidden.shape[4]
    model_width = grad_output.shape[1]
    shard_rows = down_weight.shape[1]
    raised = jnp.exp(logits)
    gating = raised / jnp.sum(raised, axis=1, keepdims=True)
    gate_sent = gating.astype(jnp.bfloat16)
    live_slot = slots < capacity
    target = jnp.where(live_slot, chosen * capacity + slots, window * capacity)
    columns = jnp.arange(window * capacity, dtype=jnp.int32)
    placing = (target[:, :, None] == columns[None, None, :]).astype(jnp.bfloat16)
    dispatch = jnp.sum(placing, axis=1)
    send_rows = jnp.einsum(
        "tr,td->rd", dispatch, grad_output, preferred_element_type=jnp.float32
    ).astype(jnp.bfloat16)
    send_gate = jnp.einsum(
        "tkr,tk->r", placing, gate_sent, preferred_element_type=jnp.float32
    ).astype(jnp.bfloat16)
    placing_float = placing.astype(jnp.float32)
    send_rows = send_rows.reshape(window, capacity, model_width)
    send_gate = send_gate.reshape(window, capacity)
    recv_rows, recv_gate = (
        lax.all_to_all(send_rows, "expert", split_axis=0, concat_axis=0, tiled=True),
        lax.all_to_all(send_gate, "expert", split_axis=0, concat_axis=0, tiled=True),
    )
    slot_rows = recv_rows.reshape(-1, model_width)
    slot_gate = recv_gate.reshape(-1).astype(jnp.float32)
    local_hidden = hidden.reshape(-1, hidden_units)
    scaled = (slot_gate[:, None] * slot_rows.astype(jnp.float32)).astype(jnp.bfloat16)
    weights = down_weight.reshape(shard_rows, model_width)
    product = lax.dot_general(
        slot_rows,
        lax.all_gather(weights, "dp", axis=0, tiled=True),
        (((1,), (1,)), ((), ())),
        preferred_element_type=jnp.float32,
    )
    grad_rows = lax.psum_scatter(
        lax.dot_general(
            local_hidden, scaled, (((0,), (0,)), ((), ())), preferred_element_type=jnp.float32
        ).astype(jnp.bfloat16),
        "dp",
        scatter_dimension=0,
        tiled=True,
    ).astype(jnp.float32)
    slot_scores = jnp.sum(local_hidden.astype(jnp.float32) * product, axis=1)
    grad_hidden = (slot_gate[:, None] * product).astype(jnp.bfloat16).reshape(hidden.shape)
    returned = lax.all_to_all(
        slot_scores.reshape(window, capacity), "expert", split_axis=0, concat_axis=0, tiled=True
    )
    token_scores = jnp.einsum(
        "tkr,r->tk", placing_float, returned.reshape(-1), precision=lax.Precision.HIGHEST
    )
    outside = jnp.where(chosen >= window, other_scores, jnp.float32(0.0))
    scores_all = jnp.where(live_slot, token_scores, outside)
    mean_score = jnp.sum(gating * scores_all, axis=1, keepdims=True)
    grad_logits = gating * (scores_all - mean_score)
    return (grad_hidden, grad_rows.reshape(1, shard_rows, model_width), grad_logits)


def body(grad_output, logits, chosen, slots, other_scores, hidden, down_weight):
    args = (grad_output, logits, chosen, slots, other_scores, hidden, down_weight)
    fits = (
        lax.axis_size("dp") % 2 == 0
        and lax.axis_size("dp") > 2
        and lax.axis_size("expert") == 4 * COLUMNS
        and hidden.shape[3] % 8 == 0
        and down_weight.shape[1] % 16 == 0
        and hidden.shape[4] % 128 == 0
        and grad_output.shape[0] == 128
        and grad_output.shape[1] % (PIECES * 128) == 0
        and logits.shape[1] == 8
    )
    return fused(*args) if fits else plain(*args)


def solution(mesh):
    placed = (
        P(("expert", "dp"), None),
        P(("expert", "dp"), None),
        P(("expert", "dp"), None),
        P(("expert", "dp"), None),
        P(("expert", "dp"), None),
        P("expert", "dp", None, None, None),
        P("expert", "dp", None),
    )
    return jax.shard_map(
        body,
        mesh=mesh,
        in_specs=placed,
        out_specs=(
            P("expert", "dp", None, None, None),
            P("expert", "dp", None),
            P(("expert", "dp"), None),
        ),
        check_vma=False,
    )
```

```python
import functools

import jax
import jax.numpy as jnp
from jax import lax
from jax.experimental import pallas as pl
from jax.experimental.pallas import tpu as pltpu
from jax.sharding import PartitionSpec as P

MESH = pl.DeviceIdType.MESH
PIECE = 256
SMALL = 128
AHEAD = 3
NEAR_AHEAD = 7
NEAR_LEAD = 3
RELAY_AHEAD = 2
PASS_AHEAD = 1
COLUMNS = 2


class Part:
    def __init__(self, p, small, count, width):
        self.p = p
        self.small = small
        if small:
            self.index, self.size = p // (count - 1), SMALL
            start = self.index * (width - SMALL)
        else:
            self.index, self.size = p - 1, PIECE
            start = SMALL + self.index * PIECE
        self.lanes = pl.ds(pl.multiple_of(start, 128), self.size)

    def of(self, pair):
        return pair[self.small].at[self.index]


def kernel(
    window, shards, capacity, ahead, near_ahead, near_lead, relay_ahead, pass_ahead, columns,
    token_hbm, logits_hbm, chosen_hbm, slots_hbm, other_hbm, hidden_hbm, weight_ref,
    gradh_ref, down_ref, logit_ref,
    token_ref, logits_ref, chosen_ref, slots_ref, other_ref, hidden_ref,
    msend, mrecv, padded, hturn, upward, tsend, trecv, gates, fmeta, fplace, lplace,
    rsend_b, rrecv_b, wfull_b, own_b, csend_b, crecv_b, ysend_b, yrecv_b, tin_b, fsend_b, lsend_b,
    rsend_s, rrecv_s, wfull_s, own_s, csend_s, crecv_s, ysend_s, yrecv_s, tin_s, fsend_s, lsend_s,
    rr, wr, dr, cr, yr, br, bo, mr, tr, qr, ws, cs, rs, ls, lh, lw, go,
):
    rsend, rrecv, wfull = (rsend_b, rsend_s), (rrecv_b, rrecv_s), (wfull_b, wfull_s)
    own, csend, crecv = (own_b, own_s), (csend_b, csend_s), (crecv_b, crecv_s)
    ysend, yrecv, tin = (ysend_b, ysend_s), (yrecv_b, yrecv_s), (tin_b, tin_s)
    fsend, lsend = (fsend_b, fsend_s), (lsend_b, lsend_s)
    me = lax.axis_index("expert")
    place = lax.axis_index("dp")
    chip, core = place // 2, place % 2
    chips = shards // 2
    mate = (me, chip * 2 + 1 - core)
    tokens, width = token_ref.shape
    count = rsend_b.shape[0] + 2
    rows = rsend_b.shape[2]
    slots_all = window * rows
    shard_rows, hidden_units = weight_ref.shape[0], hidden_ref.shape[2]

    def at(p, act):
        if isinstance(p, int):
            act(Part(p, p in (0, count - 1), count, width))
            return
        small = (p == 0) | (p == count - 1)

        @pl.when(small)
        def _():
            act(Part(p, True, count, width))

        @pl.when(jnp.logical_not(small))
        def _():
            act(Part(p, False, count, width))

    def flipped(mask):
        where = me
        for bit in range(window.bit_length() - 1):
            if mask >> bit & 1:
                where = where + (1 << bit) * (1 - 2 * (me // (1 << bit) % 2))
        return where

    level, column = me // columns, me % columns
    half, members = level // 2, window // 2
    base, far_base = half * members, (1 - half) * members
    inner = (level + 1) // 2 % 2
    side = level % 2
    own_level = side * columns
    beyond = (2 - half) * columns + column
    inward = (1 + half) * columns + column
    outward = half * 3 * columns + column
    others = [flipped(mask) for mask in range(window - 1, 0, -1)]
    near_dests = [flipped(mask) for mask in range(members - 1, 0, -1)]
    off_level = [flipped(mask) for mask in range(members - 1, columns - 1, -1)]
    beside = [flipped(mask) for mask in range(columns - 1, 0, -1)]

    def arrived(ref, sem):
        pltpu.make_async_copy(ref, ref, sem).wait()

    def settle(buffer, sem):
        arrived(buffer.at[pl.ds(0, window - 1)], sem)

    def chip_at(step):
        return lax.rem(chip + step, chips)

    def across(step):
        return (me, chip_at(step) * 2 + core)

    def remote(src, dst, send, recv, target):
        return pltpu.make_async_remote_copy(
            src_ref=src, dst_ref=dst, send_sem=send, recv_sem=recv,
            device_id=target, device_id_type=MESH,
        )

    def signal(sem, target):
        pl.semaphore_signal(sem, inc=1, device_id=target, device_id_type=MESH)

    loads = [
        pltpu.make_async_copy(src, dst, ls)
        for src, dst in (
            (chosen_hbm, chosen_ref), (slots_hbm, slots_ref), (token_hbm, token_ref),
            (logits_hbm, logits_ref), (other_hbm, other_ref),
        )
    ]
    load_hidden = pltpu.make_async_copy(hidden_hbm, hidden_ref, lh)
    for load in loads:
        load.start()
    load_hidden.start()

    barrier = pltpu.get_barrier_semaphore()
    for step in range(1, chips):
        signal(barrier, (me, chip_at(step) * 2 + 1))

    signal(barrier, mate)
    for dest in others:
        signal(barrier, (dest, chip * 2))

    def weight_copy(part, target, sem):
        return remote(weight_ref.at[:, part.lanes], part.of(wfull).at[place], ws, sem, target)

    def launch_weights(p, carry):
        def start(part):
            for step in range(1, chips):
                weight_copy(part, across(step), wr.at[p, step - 1]).start()
            weight_copy(part, mate, dr.at[p]).start()

        at(p, start)
        return carry

    @pl.when(core == 1)
    def _():
        with jax.named_scope("w_near"):
            pl.semaphore_wait(barrier, 2 * chips - 1)
        signal(go, mate)
        lax.fori_loop(0, count, launch_weights, 0)

    k = logit_ref.shape[0]
    for load in loads:
        load.wait()
    raised = jnp.exp(logits_ref[...])
    gating = raised / jnp.sum(raised, axis=0, keepdims=True)
    sent_gate = gating.astype(jnp.bfloat16).astype(jnp.float32)
    chosen = chosen_ref[...]
    slots = slots_ref[...]
    outside = jnp.where(chosen >= window, other_ref[...], 0.0)
    live = slots < capacity
    for w in range(window):
        here = live & (chosen == w)
        pos = jnp.sum(jnp.where(here, slots.astype(jnp.float32) + 1.0, 0.0), axis=0, keepdims=True) - 1.0
        gate = jnp.sum(jnp.where(here, sent_gate, 0.0), axis=0, keepdims=True)
        line = lax.broadcasted_iota(jnp.int32, (2, tokens), 0)
        msend[w] = jnp.where(line == 0, pos, gate)

    slot_id = lax.broadcasted_iota(jnp.int32, (rows, tokens), 0).astype(jnp.float32)

    def spread(ref, w):
        return slot_id == ref[w, 0:1, :]

    def placing(lines):
        return jnp.concatenate(
            [(slot_id == line).astype(jnp.float32) for line in lines], axis=0
        ).astype(jnp.bfloat16)

    dispatch = placing([msend[base + w, 0:1, :] for w in range(members)])

    def place_rows(matrix, block, experts):
        placed = jnp.dot(matrix, block, preferred_element_type=jnp.float32)
        return placed.astype(jnp.bfloat16).reshape(experts, rows, block.shape[1])

    def fill(part):
        part.of(rsend)[pl.ds(base, members)] = place_rows(dispatch, token_ref[:, part.lanes], members)

    def row_copy(part, dest):
        held = pl.ds(0, capacity)
        return remote(
            part.of(rsend).at[dest, held], part.of(rrecv).at[me, held], rs, rr.at[part.p], (dest, place)
        )

    def forward_copy(block, part, source, dest):
        held = pl.ds(0, capacity)
        return remote(
            block.at[held], part.of(rrecv).at[source, held], rs, rr.at[part.p], (dest, place)
        )

    def block_copy(part, dest, slot, sem):
        return remote(
            token_ref.at[:, part.lanes], part.of(tin).at[slot], rs, sem.at[part.p], (dest, place)
        )

    def pass_block(part):
        return remote(
            part.of(tin).at[2], part.of(tin).at[1 - side], rs, br.at[part.p], (beyond, place)
        )

    def relay_meta(first, dest, slot):
        return remote(msend.at[pl.ds(first, members)], fmeta.at[slot], rs, qr, (dest, place))

    def meta_copy(dest):
        return remote(msend.at[dest], mrecv.at[me], rs, mr, (dest, place))

    def score_copy(dest):
        return remote(tsend.at[dest], trecv.at[me], rs, tr, (dest, place))

    def pass_copy(part, slot):
        shard = part.of(wfull).at[slot]
        return remote(shard, shard, ws, dr.at[part.p], mate)

    def core_copy(part):
        return remote(part.of(csend), part.of(crecv), cs, cr.at[part.p], mate)

    def sum_copy(part, step):
        return remote(
            part.of(ysend).at[step - 1], part.of(yrecv).at[step - 1], cs, yr.at[part.p], across(step)
        )

    at(0, fill)

    @pl.when(core == 0)
    def _():
        with jax.named_scope("w_bar"):
            pl.semaphore_wait(barrier, 2 * (window - 1) + 1)
        signal(go, mate)

    @pl.when(core == 1)
    def _():
        with jax.named_scope("w_bar"):
            pl.semaphore_wait(go, 1)

    relay_meta(far_base, beyond, side).start()

    @pl.when(inner == 0)
    def _():
        relay_meta(base, inward, 2).start()

    for dest in others:
        meta_copy(dest).start()

    @pl.when(inner == 1)
    def _():
        for p in range(ahead):
            at(p, lambda part: block_copy(part, beyond, side, br).start())

    @pl.when(inner == 0)
    def _():
        for p in range(count):
            at(p, lambda part: block_copy(part, inward, 2, bo).start())

    @pl.when(core == 0)
    def _():
        with jax.named_scope("w_near"):
            pl.semaphore_wait(go, 1)
        lax.fori_loop(0, count, launch_weights, 0)

    def send_near(part):
        for dest in beside:
            row_copy(part, dest).start()

        @pl.when(inner == 1)
        def _():
            for dest in off_level:
                row_copy(part, dest).start()

    def launch(p, carry):
        @pl.when((inner == 0) | (p < near_ahead))
        def _():
            at(p, send_near)

        @pl.when(p + 1 < count)
        def _():
            at(p + 1, fill)

        return carry

    lax.fori_loop(0, count, launch, 0)

    keeps = []

    def keep_own(part):
        part.of(rrecv)[me, 0:capacity] = part.of(rsend)[me, 0:capacity]
        if rows > capacity:
            part.of(rrecv)[:, capacity:rows] = jnp.zeros(
                (window, rows - capacity, part.size), jnp.bfloat16
            )
        keeps.append(
            pltpu.make_async_copy(weight_ref.at[:, part.lanes], part.of(wfull).at[place], lw)
        )
        keeps[-1].start()

    mrecv[me] = msend[me]
    for p in range(count):
        at(p, keep_own)
    load_hidden.wait()
    padded[:, 0:capacity] = hidden_ref[...]
    if rows > capacity:
        padded[:, capacity:rows] = jnp.zeros((window, rows - capacity, hidden_units), jnp.bfloat16)
    flat = padded[...].reshape(slots_all, hidden_units)
    hturn[...] = flat.T.reshape(shards, shard_rows, slots_all)
    upward[...] = jnp.zeros_like(upward)
    for keep in keeps:
        keep.wait()

    settle(mrecv, mr)
    for s in range(window):
        gates[s] = jnp.sum(
            jnp.where(spread(mrecv, s), mrecv[s, 1:2, :], 0.0), axis=1, keepdims=True
        )

    def pump(part):
        with jax.named_scope("w_pump"):
            arrived(part.of(tin).at[2], bo.at[part.p])
        pass_block(part).start()

    def advance(part):
        block_copy(part, beyond, side, br).start()
        pump(part)

    def relay(part):
        blocks = part.of(tin)
        with jax.named_scope("w_relay"):
            arrived(blocks.at[pl.ds(0, 2)], br.at[part.p])

        @pl.when(part.p + ahead < count)
        def _():
            at(part.p + ahead, advance)

        placed, local = part.of(fsend), part.of(lsend)
        sources = [((1 - half) * 2 + i) * columns + column for i in range(2)]
        for i in range(2):
            placed[i] = place_rows(fplace[i], blocks[i], members)
        local[...] = place_rows(lplace[...], blocks[2], columns)
        for dest in near_dests:
            for i in range(2):
                forward_copy(placed.at[i, dest - base], part, sources[i], dest).start()
        for dest in beside:
            forward_copy(local.at[dest % columns], part, outward, dest).start()

        nearer = part.p + near_lead

        @pl.when((nearer >= near_ahead) & (nearer < count))
        def _():
            at(nearer, send_near)

        for i in range(2):
            part.of(rrecv)[sources[i], 0:capacity] = placed[i, me - base, 0:capacity]
        part.of(rrecv)[outward, 0:capacity] = local[column, 0:capacity]

    @pl.when(inner == 1)
    def _():
        arrived(fmeta, qr)
        for i in range(2):
            fplace[i] = placing([fmeta[i, w, 0:1, :] for w in range(members)])
        lplace[...] = placing([fmeta[2, own_level + w, 0:1, :] for w in range(columns)])
        for p in range(ahead):
            at(p, pump)
        for p in range(relay_ahead):
            at(p, relay)

    def combine(part):
        mine, came = part.of(own), part.of(crecv)
        with jax.named_scope("w_core"):
            core_copy(part).wait_recv()
        for step in range(1, chips):
            to = chip_at(step)
            part.of(ysend)[step - 1] = (mine[to] + came[to].astype(jnp.float32)).astype(jnp.bfloat16)
            sum_copy(part, step).start()
        down_ref[:, part.lanes] = mine[chip] + came[chip].astype(jnp.float32)

    def pass_weights(part):
        for step in range(1, chips):
            came = lax.rem(chip + chips - step, chips) * 2 + core
            weight_copy(part, mate, wr.at[part.p, step - 1]).wait_recv()
            pass_copy(part, came).start()

    for p in range(pass_ahead):
        at(p, pass_weights)

    def work(part):
        p = part.p

        def rows_in(remote_rows):
            with jax.named_scope("w_rows"):
                arrived(part.of(rrecv).at[pl.ds(0, remote_rows), pl.ds(0, capacity)], rr.at[p])

        @pl.when(inner == 1)
        def _():
            rows_in(window - 4)

        @pl.when(inner == 0)
        def _():
            rows_in(window - 1)

        got = part.of(rrecv)[...].reshape(slots_all, part.size)
        scaled = (gates[...].reshape(slots_all, 1) * got.astype(jnp.float32)).astype(jnp.bfloat16)
        for h in range(chips):
            part.of(csend)[h] = jnp.dot(
                hturn[2 * h + 1 - core], scaled, preferred_element_type=jnp.float32
            ).astype(jnp.bfloat16)
        core_copy(part).start()
        for h in range(chips):
            part.of(own)[h] = jnp.dot(
                hturn[2 * h + core], scaled, preferred_element_type=jnp.float32
            )
        with jax.named_scope("w_mate"):
            arrived(part.of(wfull).at[pl.ds(0, chips)], dr.at[p])
        weights = part.of(wfull)[...].reshape(hidden_units, part.size)
        upward[...] += lax.dot_general(
            got, weights, (((1,), (1,)), ((), ())), preferred_element_type=jnp.float32
        )

    def finish(p, carry):
        @pl.when((inner == 1) & (p + relay_ahead < count))
        def _():
            at(p + relay_ahead, relay)

        @pl.when(p > 0)
        def _():
            at(p - 1, combine)

        @pl.when(p + pass_ahead < count)
        def _():
            at(p + pass_ahead, pass_weights)

        at(p, work)
        return carry

    lax.fori_loop(0, count, finish, 0)
    def score_slots(dest):
        up = upward[pl.ds(pl.multiple_of(dest * rows, 16), rows)]
        score = jnp.sum(padded[dest].astype(jnp.float32) * up, axis=1, keepdims=True)
        tsend[dest] = jnp.sum(jnp.where(spread(mrecv, dest), score, 0.0), axis=0, keepdims=True)

    for dest in others[:members]:
        score_slots(dest)
        score_copy(dest).start()
    at(count - 1, combine)
    for dest in others[members:]:
        score_slots(dest)
        score_copy(dest).start()
    score_slots(me)
    trecv[me] = tsend[me]
    for s in range(window):
        up = upward[s * rows : s * rows + capacity]
        gradh_ref[s] = (gates[s, 0:capacity] * up).astype(jnp.bfloat16)

    def collect(part):
        with jax.named_scope("w_sum"):
            arrived(part.of(yrecv), yr.at[part.p])
        for step in range(1, chips):
            down_ref[:, part.lanes] += part.of(yrecv)[step - 1].astype(jnp.float32)

    held = pl.ds(0, capacity)
    for kind in range(2):
        arrived(wfull[kind].at[:, pl.ds(0, chips)], ws)
        arrived(wfull[kind].at[:, pl.ds(0, chips - 1)], ws)
        arrived(csend[kind], cs)
        arrived(rsend[kind].at[:, pl.ds(0, columns - 1), held], rs)

    @pl.when(inner == 1)
    def _():
        for kind in range(2):
            arrived(rsend[kind].at[:, pl.ds(0, members - columns), held], rs)
            arrived(tin[kind].at[:, pl.ds(0, 2)], rs)
            arrived(fsend[kind].at[:, :, pl.ds(0, members - 1), held], rs)
            arrived(lsend[kind].at[:, pl.ds(0, columns - 1), held], rs)
        arrived(msend.at[pl.ds(0, members)], rs)

    @pl.when(inner == 0)
    def _():
        for kind in range(2):
            arrived(tin[kind].at[:, 0], rs)
        arrived(msend, rs)

    settle(msend, rs)

    def collect_next(p, carry):
        at(p, collect)
        return carry

    lax.fori_loop(0, count - 1, collect_next, 0)

    with jax.named_scope("w_scores"):
        settle(trecv, tr)
    token_scores = jnp.zeros((k, tokens), jnp.float32)
    for w in range(window):
        token_scores = jnp.where(chosen == w, trecv[w], token_scores)
    scores_all = jnp.where(live, token_scores, outside)
    mean_score = jnp.sum(gating * scores_all, axis=0, keepdims=True)
    logit_ref[...] = gating * (scores_all - mean_score)
    settle(tsend, rs)

    at(count - 1, collect)
    for kind in range(2):
        arrived(ysend[kind], cs)


def write_out(a, b, c, a_out, b_out, c_out, sems):
    copies = [
        pltpu.make_async_copy(src, dst, sems.at[i])
        for i, (src, dst) in enumerate(((b, b_out), (a, a_out), (c, c_out)))
    ]
    for copy in copies:
        copy.start()
    for copy in copies:
        copy.wait()


def fused(grad_output, logits, chosen, slots, other_scores, hidden, down_weight):
    window = lax.axis_size("expert")
    shards = lax.axis_size("dp")
    capacity, hidden_units = hidden.shape[3], hidden.shape[4]
    tokens, width = grad_output.shape
    k = logits.shape[1]
    shard_rows = down_weight.shape[1]
    rows = -(-capacity // 16) * 16
    chips = shards // 2
    big = (width - 2 * SMALL) // PIECE
    count = big + 2
    vmem = pl.BlockSpec(memory_space=pltpu.VMEM)
    hbm = pl.BlockSpec(memory_space=pltpu.HBM)
    bf, f32, dma = jnp.bfloat16, jnp.float32, pltpu.SemaphoreType.DMA
    slots_all = window * rows

    def per_piece(pieces, lanes):
        return [
            pltpu.VMEM((pieces, *shape, lanes), dtype)
            for shape, dtype in (
                ((window, rows), bf),
                ((window, rows), bf),
                ((shards, shard_rows), bf),
                ((chips, shard_rows), f32),
                ((chips, shard_rows), bf),
                ((chips, shard_rows), bf),
                ((chips - 1, shard_rows), bf),
                ((chips - 1, shard_rows), bf),
                ((3, tokens), bf),
                ((2, window // 2, rows), bf),
                ((COLUMNS, rows), bf),
            )
        ]

    gradh, down, turned = pl.pallas_call(
        functools.partial(kernel, window, shards, capacity, AHEAD, NEAR_AHEAD, NEAR_LEAD, RELAY_AHEAD, PASS_AHEAD, COLUMNS),
        out_shape=(
            jax.ShapeDtypeStruct((window, capacity, hidden_units), bf),
            jax.ShapeDtypeStruct((shard_rows, width), f32),
            jax.ShapeDtypeStruct((k, tokens), f32),
        ),
        in_specs=[hbm] * 7,
        out_specs=(vmem,) * 3,
        scratch_shapes=[
            pltpu.VMEM((tokens, width), bf),
            pltpu.VMEM((k, tokens), f32),
            pltpu.VMEM((k, tokens), jnp.int32),
            pltpu.VMEM((k, tokens), jnp.int32),
            pltpu.VMEM((k, tokens), f32),
            pltpu.VMEM((window, capacity, hidden_units), bf),
            pltpu.VMEM((window, 2, tokens), f32),
            pltpu.VMEM((window, 2, tokens), f32),
            pltpu.VMEM((window, rows, hidden_units), bf),
            pltpu.VMEM((shards, shard_rows, slots_all), bf),
            pltpu.VMEM((slots_all, hidden_units), f32),
            pltpu.VMEM((window, 1, tokens), f32),
            pltpu.VMEM((window, 1, tokens), f32),
            pltpu.VMEM((window, rows, 1), f32),
            pltpu.VMEM((3, window // 2, 2, tokens), f32),
            pltpu.VMEM((2, window // 2 * rows, tokens), bf),
            pltpu.VMEM((COLUMNS * rows, tokens), bf),
            *per_piece(big, PIECE),
            *per_piece(2, SMALL),
            dma((count,)), dma((count, chips - 1)), dma((count,)), dma((count,)), dma((count,)),
            dma((count,)), dma((count,)),
            dma, dma, dma,
            dma, dma, dma,
            dma, dma, dma, pltpu.SemaphoreType.REGULAR,
        ],
        compiler_params=pltpu.CompilerParams(
            collective_id=0, has_side_effects=True, vmem_limit_bytes=48 * 1024 * 1024
        ),
    )(*(pltpu.with_memory_space_constraint(a, pltpu.HBM) for a in (
        grad_output, logits.T, chosen.T, slots.T, other_scores.T,
        hidden.reshape(window, capacity, hidden_units), down_weight.reshape(shard_rows, width),
    )))
    gradh, down, turned = (
        pltpu.with_memory_space_constraint(a, pltpu.VMEM) for a in (gradh, down, turned)
    )
    gradh, down, turned = pl.pallas_call(
        write_out,
        out_shape=tuple(jax.ShapeDtypeStruct(a.shape, a.dtype) for a in (gradh, down, turned)),
        in_specs=[vmem] * 3,
        out_specs=(hbm,) * 3,
        scratch_shapes=[dma((3,))],
        compiler_params=pltpu.CompilerParams(vmem_limit_bytes=8 * 1024 * 1024),
    )(gradh, down, turned)
    return (gradh.reshape(hidden.shape), down.reshape(1, shard_rows, width), turned.T)


def plain(grad_output, logits, chosen, slots, other_scores, hidden, down_weight):
    window = lax.axis_size("expert")
    capacity = hidden.shape[3]
    hidden_units = hidden.shape[4]
    model_width = grad_output.shape[1]
    shard_rows = down_weight.shape[1]
    raised = jnp.exp(logits)
    gating = raised / jnp.sum(raised, axis=1, keepdims=True)
    gate_sent = gating.astype(jnp.bfloat16)
    live_slot = slots < capacity
    target = jnp.where(live_slot, chosen * capacity + slots, window * capacity)
    columns = jnp.arange(window * capacity, dtype=jnp.int32)
    placing = (target[:, :, None] == columns[None, None, :]).astype(jnp.bfloat16)
    dispatch = jnp.sum(placing, axis=1)
    send_rows = jnp.einsum(
        "tr,td->rd", dispatch, grad_output, preferred_element_type=jnp.float32
    ).astype(jnp.bfloat16)
    send_gate = jnp.einsum(
        "tkr,tk->r", placing, gate_sent, preferred_element_type=jnp.float32
    ).astype(jnp.bfloat16)
    placing_float = placing.astype(jnp.float32)
    send_rows = send_rows.reshape(window, capacity, model_width)
    send_gate = send_gate.reshape(window, capacity)
    recv_rows, recv_gate = (
        lax.all_to_all(send_rows, "expert", split_axis=0, concat_axis=0, tiled=True),
        lax.all_to_all(send_gate, "expert", split_axis=0, concat_axis=0, tiled=True),
    )
    slot_rows = recv_rows.reshape(-1, model_width)
    slot_gate = recv_gate.reshape(-1).astype(jnp.float32)
    local_hidden = hidden.reshape(-1, hidden_units)
    scaled = (slot_gate[:, None] * slot_rows.astype(jnp.float32)).astype(jnp.bfloat16)
    weights = down_weight.reshape(shard_rows, model_width)
    product = lax.dot_general(
        slot_rows,
        lax.all_gather(weights, "dp", axis=0, tiled=True),
        (((1,), (1,)), ((), ())),
        preferred_element_type=jnp.float32,
    )
    grad_rows = lax.psum_scatter(
        lax.dot_general(
            local_hidden, scaled, (((0,), (0,)), ((), ())), preferred_element_type=jnp.float32
        ).astype(jnp.bfloat16),
        "dp",
        scatter_dimension=0,
        tiled=True,
    ).astype(jnp.float32)
    slot_scores = jnp.sum(local_hidden.astype(jnp.float32) * product, axis=1)
    grad_hidden = (slot_gate[:, None] * product).astype(jnp.bfloat16).reshape(hidden.shape)
    returned = lax.all_to_all(
        slot_scores.reshape(window, capacity), "expert", split_axis=0, concat_axis=0, tiled=True
    )
    token_scores = jnp.einsum(
        "tkr,r->tk", placing_float, returned.reshape(-1), precision=lax.Precision.HIGHEST
    )
    outside = jnp.where(chosen >= window, other_scores, jnp.float32(0.0))
    scores_all = jnp.where(live_slot, token_scores, outside)
    mean_score = jnp.sum(gating * scores_all, axis=1, keepdims=True)
    grad_logits = gating * (scores_all - mean_score)
    return (grad_hidden, grad_rows.reshape(1, shard_rows, model_width), grad_logits)


def body(grad_output, logits, chosen, slots, other_scores, hidden, down_weight):
    args = (grad_output, logits, chosen, slots, other_scores, hidden, down_weight)
    fits = (
        lax.axis_size("dp") % 2 == 0
        and lax.axis_size("dp") > 2
        and lax.axis_size("expert") == 4 * COLUMNS
        and hidden.shape[3] % 8 == 0
        and down_weight.shape[1] % 16 == 0
        and hidden.shape[4] % 128 == 0
        and grad_output.shape[0] == 128
        and grad_output.shape[1] % PIECE == 0
        and grad_output.shape[1] >= 2 * SMALL + 3 * PIECE
        and logits.shape[1] == 8
    )
    return fused(*args) if fits else plain(*args)


def solution(mesh):
    placed = (
        P(("expert", "dp"), None),
        P(("expert", "dp"), None),
        P(("expert", "dp"), None),
        P(("expert", "dp"), None),
        P(("expert", "dp"), None),
        P("expert", "dp", None, None, None),
        P("expert", "dp", None),
    )
    return jax.shard_map(
        body,
        mesh=mesh,
        in_specs=placed,
        out_specs=(
            P("expert", "dp", None, None, None),
            P("expert", "dp", None),
            P(("expert", "dp"), None),
        ),
        check_vma=False,
    )
```

```python
import functools

import jax
import jax.numpy as jnp
from jax import lax
from jax.experimental import pallas as pl
from jax.experimental.pallas import tpu as pltpu
from jax.sharding import PartitionSpec as P

MESH = pl.DeviceIdType.MESH
PIECE = 256
SMALL = 128
HEADS = 1
TAILS = 3
AHEAD = 3
NEAR_AHEAD = 7
NEAR_LEAD = 3
RELAY_AHEAD = 2
PASS_AHEAD = 1
COLUMNS = 2


class Part:
    def __init__(self, p, small, big):
        self.p = p
        self.small = small
        past = p // (HEADS + big)
        if small:
            self.index, self.size = p - big * past, SMALL
            start = self.index * SMALL + past * (big * PIECE)
        else:
            self.index, self.size = p - HEADS, PIECE
            start = HEADS * SMALL + self.index * PIECE
        self.lanes = pl.ds(pl.multiple_of(start, 128), self.size)

    def of(self, pair):
        return pair[self.small].at[self.index]


def kernel(
    window, shards, capacity, ahead, near_ahead, near_lead, relay_ahead, pass_ahead, columns,
    token_hbm, logits_hbm, chosen_hbm, slots_hbm, other_hbm, hidden_hbm, weight_ref,
    gradh_ref, down_ref, logit_ref,
    token_ref, logits_ref, chosen_ref, slots_ref, other_ref, hidden_ref,
    msend, mrecv, padded, hturn, upward, tsend, trecv, gates, fmeta, fplace, lplace,
    rsend_b, rrecv_b, wfull_b, own_b, csend_b, crecv_b, ysend_b, yrecv_b, tin_b, fsend_b, lsend_b,
    rsend_s, rrecv_s, wfull_s, own_s, csend_s, crecv_s, ysend_s, yrecv_s, tin_s, fsend_s, lsend_s,
    rr, wr, dr, cr, yr, br, bo, mr, tr, qr, ws, cs, rs, ls, lh, lw, go,
):
    rsend, rrecv, wfull = (rsend_b, rsend_s), (rrecv_b, rrecv_s), (wfull_b, wfull_s)
    own, csend, crecv = (own_b, own_s), (csend_b, csend_s), (crecv_b, crecv_s)
    ysend, yrecv, tin = (ysend_b, ysend_s), (yrecv_b, yrecv_s), (tin_b, tin_s)
    fsend, lsend = (fsend_b, fsend_s), (lsend_b, lsend_s)
    me = lax.axis_index("expert")
    place = lax.axis_index("dp")
    chip, core = place // 2, place % 2
    chips = shards // 2
    mate = (me, chip * 2 + 1 - core)
    tokens, width = token_ref.shape
    big = rsend_b.shape[0]
    count = HEADS + big + TAILS
    rows = rsend_b.shape[2]
    slots_all = window * rows
    shard_rows, hidden_units = weight_ref.shape[0], hidden_ref.shape[2]

    def at(p, act):
        if isinstance(p, int):
            act(Part(p, p < HEADS or p >= HEADS + big, big))
            return
        small = (p < HEADS) | (p >= HEADS + big)

        @pl.when(small)
        def _():
            act(Part(p, True, big))

        @pl.when(jnp.logical_not(small))
        def _():
            act(Part(p, False, big))

    def flipped(mask):
        where = me
        for bit in range(window.bit_length() - 1):
            if mask >> bit & 1:
                where = where + (1 << bit) * (1 - 2 * (me // (1 << bit) % 2))
        return where

    level, column = me // columns, me % columns
    half, members = level // 2, window // 2
    base, far_base = half * members, (1 - half) * members
    inner = (level + 1) // 2 % 2
    side = level % 2
    own_level = side * columns
    beyond = (2 - half) * columns + column
    inward = (1 + half) * columns + column
    outward = half * 3 * columns + column
    others = [flipped(mask) for mask in range(window - 1, 0, -1)]
    near_dests = [flipped(mask) for mask in range(members - 1, 0, -1)]
    off_level = [flipped(mask) for mask in range(members - 1, columns - 1, -1)]
    beside = [flipped(mask) for mask in range(columns - 1, 0, -1)]

    def arrived(ref, sem):
        pltpu.make_async_copy(ref, ref, sem).wait()

    def settle(buffer, sem):
        arrived(buffer.at[pl.ds(0, window - 1)], sem)

    def chip_at(step):
        return lax.rem(chip + step, chips)

    def across(step):
        return (me, chip_at(step) * 2 + core)

    def remote(src, dst, send, recv, target):
        return pltpu.make_async_remote_copy(
            src_ref=src, dst_ref=dst, send_sem=send, recv_sem=recv,
            device_id=target, device_id_type=MESH,
        )

    def signal(sem, target):
        pl.semaphore_signal(sem, inc=1, device_id=target, device_id_type=MESH)

    loads = [
        pltpu.make_async_copy(src, dst, ls)
        for src, dst in (
            (chosen_hbm, chosen_ref), (slots_hbm, slots_ref), (token_hbm, token_ref),
            (logits_hbm, logits_ref), (other_hbm, other_ref),
        )
    ]
    load_hidden = pltpu.make_async_copy(hidden_hbm, hidden_ref, lh)
    for load in loads:
        load.start()
    load_hidden.start()

    barrier = pltpu.get_barrier_semaphore()
    for step in range(1, chips):
        signal(barrier, (me, chip_at(step) * 2 + 1))

    signal(barrier, mate)
    for dest in others:
        signal(barrier, (dest, chip * 2))

    def weight_copy(part, target, sem):
        return remote(weight_ref.at[:, part.lanes], part.of(wfull).at[place], ws, sem, target)

    def launch_weights(p, carry):
        def start(part):
            for step in range(1, chips):
                weight_copy(part, across(step), wr.at[p, step - 1]).start()
            weight_copy(part, mate, dr.at[p]).start()

        at(p, start)
        return carry

    @pl.when(core == 1)
    def _():
        with jax.named_scope("w_near"):
            pl.semaphore_wait(barrier, 2 * chips - 1)
        signal(go, mate)
        lax.fori_loop(0, count, launch_weights, 0)

    k = logit_ref.shape[0]
    for load in loads:
        load.wait()
    raised = jnp.exp(logits_ref[...])
    gating = raised / jnp.sum(raised, axis=0, keepdims=True)
    sent_gate = gating.astype(jnp.bfloat16).astype(jnp.float32)
    chosen = chosen_ref[...]
    slots = slots_ref[...]
    outside = jnp.where(chosen >= window, other_ref[...], 0.0)
    live = slots < capacity
    for w in range(window):
        here = live & (chosen == w)
        pos = jnp.sum(jnp.where(here, slots.astype(jnp.float32) + 1.0, 0.0), axis=0, keepdims=True) - 1.0
        gate = jnp.sum(jnp.where(here, sent_gate, 0.0), axis=0, keepdims=True)
        line = lax.broadcasted_iota(jnp.int32, (2, tokens), 0)
        msend[w] = jnp.where(line == 0, pos, gate)

    slot_id = lax.broadcasted_iota(jnp.int32, (rows, tokens), 0).astype(jnp.float32)

    def spread(ref, w):
        return slot_id == ref[w, 0:1, :]

    def placing(lines):
        return jnp.concatenate(
            [(slot_id == line).astype(jnp.float32) for line in lines], axis=0
        ).astype(jnp.bfloat16)

    dispatch = placing([msend[base + w, 0:1, :] for w in range(members)])

    def place_rows(matrix, block, experts):
        placed = jnp.dot(matrix, block, preferred_element_type=jnp.float32)
        return placed.astype(jnp.bfloat16).reshape(experts, rows, block.shape[1])

    def fill(part):
        part.of(rsend)[pl.ds(base, members)] = place_rows(dispatch, token_ref[:, part.lanes], members)

    def row_copy(part, dest):
        held = pl.ds(0, capacity)
        return remote(
            part.of(rsend).at[dest, held], part.of(rrecv).at[me, held], rs, rr.at[part.p], (dest, place)
        )

    def forward_copy(block, part, source, dest):
        held = pl.ds(0, capacity)
        return remote(
            block.at[held], part.of(rrecv).at[source, held], rs, rr.at[part.p], (dest, place)
        )

    def block_copy(part, dest, slot, sem):
        return remote(
            token_ref.at[:, part.lanes], part.of(tin).at[slot], rs, sem.at[part.p], (dest, place)
        )

    def pass_block(part):
        return remote(
            part.of(tin).at[2], part.of(tin).at[1 - side], rs, br.at[part.p], (beyond, place)
        )

    def relay_meta(first, dest, slot):
        return remote(msend.at[pl.ds(first, members)], fmeta.at[slot], rs, qr, (dest, place))

    def meta_copy(dest):
        return remote(msend.at[dest], mrecv.at[me], rs, mr, (dest, place))

    def score_copy(dest):
        return remote(tsend.at[dest], trecv.at[me], rs, tr, (dest, place))

    def pass_copy(part, slot):
        shard = part.of(wfull).at[slot]
        return remote(shard, shard, ws, dr.at[part.p], mate)

    def core_copy(part):
        return remote(part.of(csend), part.of(crecv), cs, cr.at[part.p], mate)

    def sum_copy(part, step):
        mark = 1 + (part.p + 1) // count if part.small else 0
        return remote(
            part.of(ysend).at[step - 1], part.of(yrecv).at[step - 1], cs, yr.at[mark], across(step)
        )

    at(0, fill)

    @pl.when(core == 0)
    def _():
        with jax.named_scope("w_bar"):
            pl.semaphore_wait(barrier, 2 * (window - 1) + 1)
        signal(go, mate)

    @pl.when(core == 1)
    def _():
        with jax.named_scope("w_bar"):
            pl.semaphore_wait(go, 1)

    relay_meta(far_base, beyond, side).start()

    @pl.when(inner == 0)
    def _():
        relay_meta(base, inward, 2).start()

    for dest in others:
        meta_copy(dest).start()

    @pl.when(inner == 1)
    def _():
        for p in range(ahead):
            at(p, lambda part: block_copy(part, beyond, side, br).start())

    @pl.when(inner == 0)
    def _():
        for p in range(count):
            at(p, lambda part: block_copy(part, inward, 2, bo).start())

    @pl.when(core == 0)
    def _():
        with jax.named_scope("w_near"):
            pl.semaphore_wait(go, 1)
        lax.fori_loop(0, count, launch_weights, 0)

    def send_near(part):
        for dest in beside:
            row_copy(part, dest).start()

        @pl.when(inner == 1)
        def _():
            for dest in off_level:
                row_copy(part, dest).start()

    def launch(p, carry):
        @pl.when((inner == 0) | (p < near_ahead))
        def _():
            at(p, send_near)

        @pl.when(p + 1 < count)
        def _():
            at(p + 1, fill)

        return carry

    lax.fori_loop(0, count, launch, 0)

    keeps = []

    def keep_own(part):
        part.of(rrecv)[me, 0:capacity] = part.of(rsend)[me, 0:capacity]
        if rows > capacity:
            part.of(rrecv)[:, capacity:rows] = jnp.zeros(
                (window, rows - capacity, part.size), jnp.bfloat16
            )
        keeps.append(
            pltpu.make_async_copy(weight_ref.at[:, part.lanes], part.of(wfull).at[place], lw)
        )
        keeps[-1].start()

    mrecv[me] = msend[me]
    for p in range(count):
        at(p, keep_own)
    load_hidden.wait()
    padded[:, 0:capacity] = hidden_ref[...]
    if rows > capacity:
        padded[:, capacity:rows] = jnp.zeros((window, rows - capacity, hidden_units), jnp.bfloat16)
    flat = padded[...].reshape(slots_all, hidden_units)
    hturn[...] = flat.T.reshape(shards, shard_rows, slots_all)
    upward[...] = jnp.zeros_like(upward)
    for keep in keeps:
        keep.wait()

    settle(mrecv, mr)
    for s in range(window):
        gates[s] = jnp.sum(
            jnp.where(spread(mrecv, s), mrecv[s, 1:2, :], 0.0), axis=1, keepdims=True
        )

    def pump(part):
        with jax.named_scope("w_pump"):
            arrived(part.of(tin).at[2], bo.at[part.p])
        pass_block(part).start()

    def advance(part):
        block_copy(part, beyond, side, br).start()
        pump(part)

    def relay(part):
        blocks = part.of(tin)
        with jax.named_scope("w_relay"):
            arrived(blocks.at[pl.ds(0, 2)], br.at[part.p])

        @pl.when(part.p + ahead < count)
        def _():
            at(part.p + ahead, advance)

        placed, local = part.of(fsend), part.of(lsend)
        sources = [((1 - half) * 2 + i) * columns + column for i in range(2)]
        for i in range(2):
            placed[i] = place_rows(fplace[i], blocks[i], members)
        local[...] = place_rows(lplace[...], blocks[2], columns)
        for dest in near_dests:
            for i in range(2):
                forward_copy(placed.at[i, dest - base], part, sources[i], dest).start()
        for dest in beside:
            forward_copy(local.at[dest % columns], part, outward, dest).start()

        nearer = part.p + near_lead

        @pl.when((nearer >= near_ahead) & (nearer < count))
        def _():
            at(nearer, send_near)

        for i in range(2):
            part.of(rrecv)[sources[i], 0:capacity] = placed[i, me - base, 0:capacity]
        part.of(rrecv)[outward, 0:capacity] = local[column, 0:capacity]

    @pl.when(inner == 1)
    def _():
        arrived(fmeta, qr)
        for i in range(2):
            fplace[i] = placing([fmeta[i, w, 0:1, :] for w in range(members)])
        lplace[...] = placing([fmeta[2, own_level + w, 0:1, :] for w in range(columns)])
        for p in range(ahead):
            at(p, pump)
        for p in range(relay_ahead):
            at(p, relay)

    def combine(part):
        mine, came = part.of(own), part.of(crecv)
        with jax.named_scope("w_core"):
            core_copy(part).wait_recv()
        for step in range(1, chips):
            to = chip_at(step)
            part.of(ysend)[step - 1] = (mine[to] + came[to].astype(jnp.float32)).astype(jnp.bfloat16)
            sum_copy(part, step).start()
        down_ref[:, part.lanes] = mine[chip] + came[chip].astype(jnp.float32)

    def pass_weights(part):
        for step in range(1, chips):
            came = lax.rem(chip + chips - step, chips) * 2 + core
            weight_copy(part, mate, wr.at[part.p, step - 1]).wait_recv()
            pass_copy(part, came).start()

    for p in range(pass_ahead):
        at(p, pass_weights)

    def lift(part):
        got = part.of(rrecv)[...].reshape(slots_all, part.size)
        with jax.named_scope("w_mate"):
            arrived(part.of(wfull).at[pl.ds(0, chips)], dr.at[part.p])
        weights = part.of(wfull)[...].reshape(hidden_units, part.size)
        upward[...] += lax.dot_general(
            got, weights, (((1,), (1,)), ((), ())), preferred_element_type=jnp.float32
        )

    def work(part):
        p = part.p

        def rows_in(remote_rows):
            with jax.named_scope("w_rows"):
                arrived(part.of(rrecv).at[pl.ds(0, remote_rows), pl.ds(0, capacity)], rr.at[p])

        @pl.when(inner == 1)
        def _():
            rows_in(window - 4)

        @pl.when(inner == 0)
        def _():
            rows_in(window - 1)

        @pl.when(p + 1 == count)
        def _():
            lift(part)

        got = part.of(rrecv)[...].reshape(slots_all, part.size)
        scaled = (gates[...].reshape(slots_all, 1) * got.astype(jnp.float32)).astype(jnp.bfloat16)
        for h in range(chips):
            part.of(csend)[h] = jnp.dot(
                hturn[2 * h + 1 - core], scaled, preferred_element_type=jnp.float32
            ).astype(jnp.bfloat16)
        core_copy(part).start()
        for h in range(chips):
            part.of(own)[h] = jnp.dot(
                hturn[2 * h + core], scaled, preferred_element_type=jnp.float32
            )
        @pl.when(p + 1 < count)
        def _():
            lift(part)

    def finish(p, carry):
        @pl.when((inner == 1) & (p + relay_ahead < count))
        def _():
            at(p + relay_ahead, relay)

        @pl.when(p > 0)
        def _():
            at(p - 1, combine)

        @pl.when(p + pass_ahead < count)
        def _():
            at(p + pass_ahead, pass_weights)

        at(p, work)
        return carry

    lax.fori_loop(0, count, finish, 0)
    def score_slots(dest):
        up = upward[pl.ds(pl.multiple_of(dest * rows, 16), rows)]
        score = jnp.sum(padded[dest].astype(jnp.float32) * up, axis=1, keepdims=True)
        tsend[dest] = jnp.sum(jnp.where(spread(mrecv, dest), score, 0.0), axis=0, keepdims=True)

    for dest in others[:members]:
        score_slots(dest)
        score_copy(dest).start()
    at(count - 1, combine)
    for dest in others[members:]:
        score_slots(dest)
        score_copy(dest).start()
    score_slots(me)
    trecv[me] = tsend[me]
    for s in range(window):
        up = upward[s * rows : s * rows + capacity]
        gradh_ref[s] = (gates[s, 0:capacity] * up).astype(jnp.bfloat16)

    def collect(part):
        for step in range(1, chips):
            down_ref[:, part.lanes] += part.of(yrecv)[step - 1].astype(jnp.float32)

    held = pl.ds(0, capacity)
    for kind in range(2):
        arrived(wfull[kind].at[:, pl.ds(0, chips)], ws)
        arrived(wfull[kind].at[:, pl.ds(0, chips - 1)], ws)
        arrived(csend[kind], cs)
        arrived(rsend[kind].at[:, pl.ds(0, columns - 1), held], rs)

    @pl.when(inner == 1)
    def _():
        for kind in range(2):
            arrived(rsend[kind].at[:, pl.ds(0, members - columns), held], rs)
            arrived(tin[kind].at[:, pl.ds(0, 2)], rs)
            arrived(fsend[kind].at[:, :, pl.ds(0, members - 1), held], rs)
            arrived(lsend[kind].at[:, pl.ds(0, columns - 1), held], rs)
        arrived(msend.at[pl.ds(0, members)], rs)

    @pl.when(inner == 0)
    def _():
        for kind in range(2):
            arrived(tin[kind].at[:, 0], rs)
        arrived(msend, rs)

    settle(msend, rs)

    def collect_next(p, carry):
        at(p, collect)
        return carry

    with jax.named_scope("w_sums"):
        arrived(yrecv_b, yr.at[0])
        arrived(yrecv_s.at[pl.ds(0, HEADS + TAILS - 1)], yr.at[1])
    lax.fori_loop(0, count - 1, collect_next, 0)

    with jax.named_scope("w_scores"):
        settle(trecv, tr)
    token_scores = jnp.zeros((k, tokens), jnp.float32)
    for w in range(window):
        token_scores = jnp.where(chosen == w, trecv[w], token_scores)
    scores_all = jnp.where(live, token_scores, outside)
    mean_score = jnp.sum(gating * scores_all, axis=0, keepdims=True)
    logit_ref[...] = gating * (scores_all - mean_score)
    settle(tsend, rs)

    with jax.named_scope("w_sum"):
        arrived(yrecv_s.at[HEADS + TAILS - 1], yr.at[2])
    at(count - 1, collect)
    for kind in range(2):
        arrived(ysend[kind], cs)


def write_out(a, b, c, a_out, b_out, c_out, sems):
    copies = [
        pltpu.make_async_copy(src, dst, sems.at[i])
        for i, (src, dst) in enumerate(((b, b_out), (a, a_out), (c, c_out)))
    ]
    for copy in copies:
        copy.start()
    for copy in copies:
        copy.wait()


def fused(grad_output, logits, chosen, slots, other_scores, hidden, down_weight):
    window = lax.axis_size("expert")
    shards = lax.axis_size("dp")
    capacity, hidden_units = hidden.shape[3], hidden.shape[4]
    tokens, width = grad_output.shape
    k = logits.shape[1]
    shard_rows = down_weight.shape[1]
    rows = -(-capacity // 16) * 16
    chips = shards // 2
    ends = HEADS + TAILS
    big = (width - ends * SMALL) // PIECE
    count = big + ends
    vmem = pl.BlockSpec(memory_space=pltpu.VMEM)
    hbm = pl.BlockSpec(memory_space=pltpu.HBM)
    bf, f32, dma = jnp.bfloat16, jnp.float32, pltpu.SemaphoreType.DMA
    slots_all = window * rows

    def per_piece(pieces, lanes):
        return [
            pltpu.VMEM((pieces, *shape, lanes), dtype)
            for shape, dtype in (
                ((window, rows), bf),
                ((window, rows), bf),
                ((shards, shard_rows), bf),
                ((chips, shard_rows), f32),
                ((chips, shard_rows), bf),
                ((chips, shard_rows), bf),
                ((chips - 1, shard_rows), bf),
                ((chips - 1, shard_rows), bf),
                ((3, tokens), bf),
                ((2, window // 2, rows), bf),
                ((COLUMNS, rows), bf),
            )
        ]

    gradh, down, turned = pl.pallas_call(
        functools.partial(kernel, window, shards, capacity, AHEAD, NEAR_AHEAD, NEAR_LEAD, RELAY_AHEAD, PASS_AHEAD, COLUMNS),
        out_shape=(
            jax.ShapeDtypeStruct((window, capacity, hidden_units), bf),
            jax.ShapeDtypeStruct((shard_rows, width), f32),
            jax.ShapeDtypeStruct((k, tokens), f32),
        ),
        in_specs=[hbm] * 7,
        out_specs=(vmem,) * 3,
        scratch_shapes=[
            pltpu.VMEM((tokens, width), bf),
            pltpu.VMEM((k, tokens), f32),
            pltpu.VMEM((k, tokens), jnp.int32),
            pltpu.VMEM((k, tokens), jnp.int32),
            pltpu.VMEM((k, tokens), f32),
            pltpu.VMEM((window, capacity, hidden_units), bf),
            pltpu.VMEM((window, 2, tokens), f32),
            pltpu.VMEM((window, 2, tokens), f32),
            pltpu.VMEM((window, rows, hidden_units), bf),
            pltpu.VMEM((shards, shard_rows, slots_all), bf),
            pltpu.VMEM((slots_all, hidden_units), f32),
            pltpu.VMEM((window, 1, tokens), f32),
            pltpu.VMEM((window, 1, tokens), f32),
            pltpu.VMEM((window, rows, 1), f32),
            pltpu.VMEM((3, window // 2, 2, tokens), f32),
            pltpu.VMEM((2, window // 2 * rows, tokens), bf),
            pltpu.VMEM((COLUMNS * rows, tokens), bf),
            *per_piece(big, PIECE),
            *per_piece(ends, SMALL),
            dma((count,)), dma((count, chips - 1)), dma((count,)), dma((count,)), dma((3,)),
            dma((count,)), dma((count,)),
            dma, dma, dma,
            dma, dma, dma,
            dma, dma, dma, pltpu.SemaphoreType.REGULAR,
        ],
        compiler_params=pltpu.CompilerParams(
            collective_id=0, has_side_effects=True, vmem_limit_bytes=48 * 1024 * 1024
        ),
    )(*(pltpu.with_memory_space_constraint(a, pltpu.HBM) for a in (
        grad_output, logits.T, chosen.T, slots.T, other_scores.T,
        hidden.reshape(window, capacity, hidden_units), down_weight.reshape(shard_rows, width),
    )))
    gradh, down, turned = (
        pltpu.with_memory_space_constraint(a, pltpu.VMEM) for a in (gradh, down, turned)
    )
    gradh, down, turned = pl.pallas_call(
        write_out,
        out_shape=tuple(jax.ShapeDtypeStruct(a.shape, a.dtype) for a in (gradh, down, turned)),
        in_specs=[vmem] * 3,
        out_specs=(hbm,) * 3,
        scratch_shapes=[dma((3,))],
        compiler_params=pltpu.CompilerParams(vmem_limit_bytes=8 * 1024 * 1024),
    )(gradh, down, turned)
    return (gradh.reshape(hidden.shape), down.reshape(1, shard_rows, width), turned.T)


def plain(grad_output, logits, chosen, slots, other_scores, hidden, down_weight):
    window = lax.axis_size("expert")
    capacity = hidden.shape[3]
    hidden_units = hidden.shape[4]
    model_width = grad_output.shape[1]
    shard_rows = down_weight.shape[1]
    raised = jnp.exp(logits)
    gating = raised / jnp.sum(raised, axis=1, keepdims=True)
    gate_sent = gating.astype(jnp.bfloat16)
    live_slot = slots < capacity
    target = jnp.where(live_slot, chosen * capacity + slots, window * capacity)
    columns = jnp.arange(window * capacity, dtype=jnp.int32)
    placing = (target[:, :, None] == columns[None, None, :]).astype(jnp.bfloat16)
    dispatch = jnp.sum(placing, axis=1)
    send_rows = jnp.einsum(
        "tr,td->rd", dispatch, grad_output, preferred_element_type=jnp.float32
    ).astype(jnp.bfloat16)
    send_gate = jnp.einsum(
        "tkr,tk->r", placing, gate_sent, preferred_element_type=jnp.float32
    ).astype(jnp.bfloat16)
    placing_float = placing.astype(jnp.float32)
    send_rows = send_rows.reshape(window, capacity, model_width)
    send_gate = send_gate.reshape(window, capacity)
    recv_rows, recv_gate = (
        lax.all_to_all(send_rows, "expert", split_axis=0, concat_axis=0, tiled=True),
        lax.all_to_all(send_gate, "expert", split_axis=0, concat_axis=0, tiled=True),
    )
    slot_rows = recv_rows.reshape(-1, model_width)
    slot_gate = recv_gate.reshape(-1).astype(jnp.float32)
    local_hidden = hidden.reshape(-1, hidden_units)
    scaled = (slot_gate[:, None] * slot_rows.astype(jnp.float32)).astype(jnp.bfloat16)
    weights = down_weight.reshape(shard_rows, model_width)
    product = lax.dot_general(
        slot_rows,
        lax.all_gather(weights, "dp", axis=0, tiled=True),
        (((1,), (1,)), ((), ())),
        preferred_element_type=jnp.float32,
    )
    grad_rows = lax.psum_scatter(
        lax.dot_general(
            local_hidden, scaled, (((0,), (0,)), ((), ())), preferred_element_type=jnp.float32
        ).astype(jnp.bfloat16),
        "dp",
        scatter_dimension=0,
        tiled=True,
    ).astype(jnp.float32)
    slot_scores = jnp.sum(local_hidden.astype(jnp.float32) * product, axis=1)
    grad_hidden = (slot_gate[:, None] * product).astype(jnp.bfloat16).reshape(hidden.shape)
    returned = lax.all_to_all(
        slot_scores.reshape(window, capacity), "expert", split_axis=0, concat_axis=0, tiled=True
    )
    token_scores = jnp.einsum(
        "tkr,r->tk", placing_float, returned.reshape(-1), precision=lax.Precision.HIGHEST
    )
    outside = jnp.where(chosen >= window, other_scores, jnp.float32(0.0))
    scores_all = jnp.where(live_slot, token_scores, outside)
    mean_score = jnp.sum(gating * scores_all, axis=1, keepdims=True)
    grad_logits = gating * (scores_all - mean_score)
    return (grad_hidden, grad_rows.reshape(1, shard_rows, model_width), grad_logits)


def body(grad_output, logits, chosen, slots, other_scores, hidden, down_weight):
    args = (grad_output, logits, chosen, slots, other_scores, hidden, down_weight)
    fits = (
        lax.axis_size("dp") % 2 == 0
        and lax.axis_size("dp") > 2
        and lax.axis_size("expert") == 4 * COLUMNS
        and hidden.shape[3] % 8 == 0
        and down_weight.shape[1] % 16 == 0
        and hidden.shape[4] % 128 == 0
        and grad_output.shape[0] == 128
        and (grad_output.shape[1] - (HEADS + TAILS) * SMALL) % PIECE == 0
        and grad_output.shape[1] >= (HEADS + TAILS) * SMALL + 4 * PIECE
        and logits.shape[1] == 8
    )
    return fused(*args) if fits else plain(*args)


def solution(mesh):
    placed = (
        P(("expert", "dp"), None),
        P(("expert", "dp"), None),
        P(("expert", "dp"), None),
        P(("expert", "dp"), None),
        P(("expert", "dp"), None),
        P("expert", "dp", None, None, None),
        P("expert", "dp", None),
    )
    return jax.shard_map(
        body,
        mesh=mesh,
        in_specs=placed,
        out_specs=(
            P("expert", "dp", None, None, None),
            P("expert", "dp", None),
            P(("expert", "dp"), None),
        ),
        check_vma=False,
    )
```
